256 devices in a mesh: scen: 2 (over z), gx: 128 (over y, x, core).
Axes of the slice: x: 8, y: 8, z: 2, core: 2. Of those that a mesh axis runs over, the one named last changes fastest.
The devices are a block of a 8x8x16 slice.
Arguments:
- populations: float32 [54, 128, 4, 8, 256], P('scen', 'gx'), parts along dimension 0, may hold values from 0.15 to 2
- cell_kind: int32 [128, 4, 8, 512], P('gx', None, None, 'scen'), parts along dimension 3, may hold values from 0 to 4, as said below
- profile: int32 [128, 4, 8, 512], P('gx', None, None, 'scen'), parts along dimension 3, may hold values from 0 to 7
- vent_table: float32 [16, 3], P('scen'), parts along dimension 0, may hold values from -0.08 to 0.08
- rates: float32 [27], replicated, may hold values from 1 to 1.9
Outputs:
- advanced: float32 [54, 128, 4, 8, 256], P('scen', 'gx'), parts along dimension 0
The draws below stay inside these ranges and needn't reach their ends.
There are 2 independent parts, one for each index of `scen`. The reference program is written for one: setup_inputs(seed, part) draws one part's arguments, and reference() takes and returns one part's arrays. A program takes and returns all parts, laid end to end along the dimension named above; an argument that names none is the same for every part. Nothing has to cross between parts.
Inputs may be any that keep to these rules, and one draw needn't show every extreme that they name: `cell_kind`: 0 fluid, 1 wall, 2 vent, 3 inflow, 4 outflow.
All inputs are finite; a program needn't handle non-finite values.
Results may differ from the reference program's by a relative error of at most 0.0003.
Values sent between devices are 32-bit elements; how exact they have to be, the bound alone decides.
A program may use at most 64 MiB of HBM per device.

```python
import jax
import jax.numpy as jnp
import numpy as np
from jax import lax

PY = 8
CX = 4
CY = 8
NZ = 256
STEPS = 3
PROFILES = 8
BLOCKS = 128


def draw_populations(key, part):
    first_key, second_key, third_key = jax.random.split(key, 3)
    velocity = jnp.clip(jax.random.normal(first_key, (3, BLOCKS, CX, CY, NZ), jnp.float32) * 0.03, -0.05, 0.05)
    density = 1.0 + jax.random.uniform(third_key, (BLOCKS, CX, CY, NZ), jnp.float32, -0.1, 0.1)
    deviation = jnp.clip(jax.random.normal(second_key, (27, BLOCKS, CX, CY, NZ), jnp.float32) * 0.12, -0.3, 0.3)
    columns = []
    for k in range(27):
        step_x = float(k // 9 - 1)
        step_y = float(k // 3 % 3 - 1)
        step_z = float(k % 3 - 1)
        projected = step_x * velocity[0] + step_y * velocity[1] + step_z * velocity[2]
        columns.append(density * (1.0 + 3.0 * projected))
    return jnp.stack(columns) + deviation


def draw_cell_kind(key, part):
    ticket = jax.random.randint(key, (BLOCKS, CX, CY, NZ), 0, 100)
    return jnp.where(ticket < 70, 0, jnp.where(ticket < 80, 1, jnp.where(ticket < 88, 2, jnp.where(ticket < 94, 3, 4)))).astype(jnp.int32)


def with_ends(drawn, own_key, least, high):
    spot = [jax.random.randint(jax.random.fold_in(own_key, axis), (), 0, length) for axis, length in enumerate(drawn.shape)]
    longest = drawn.shape.index(max(drawn.shape))
    neighbour = spot[:longest] + [(spot[longest] + 1) % drawn.shape[longest]] + spot[longest + 1:]
    return drawn.at[tuple(spot)].set(least).at[tuple(neighbour)].set(high)


def setup_inputs(seed: int = 0, part: int = 0) -> dict:
    key_of = jax.random.split(jax.random.key(seed), 6)
    part_keys = jax.random.split(jax.random.fold_in(key_of[5], part), 6)
    return {
        "populations": draw_populations(jax.random.fold_in(jax.random.fold_in(key_of[5], part), 71), part),
        "cell_kind": draw_cell_kind(jax.random.fold_in(jax.random.fold_in(key_of[5], part), 71), part),
        "profile": with_ends(jax.random.randint(part_keys[2], (BLOCKS, CX, CY, NZ), 0, PROFILES), jax.random.fold_in(part_keys[2], 1), 0, PROFILES - 1).astype(jnp.int32),
        "vent_table": jnp.clip(jax.random.uniform(part_keys[3], (PROFILES, 3), jnp.float32, -0.08, 0.08), -0.08, 0.08),
        "rates": jnp.clip(jax.random.uniform(key_of[4], (27,), jnp.float32, 1.0, 1.9), 1.0, 1.9),
    }


def lattice_tables():
    speeds = np.array([[a - 1.0, b - 1.0, d - 1.0] for a in range(3) for b in range(3) for d in range(3)])
    single = np.array([1.0 / 6.0, 2.0 / 3.0, 1.0 / 6.0])
    weights = np.kron(np.kron(single, single), single)
    powers = np.array([[1.0, 1.0, 1.0], [-1.0, 0.0, 1.0], [1.0, 0.0, 1.0]])
    undo = np.array([[0.0, -0.5, 0.5], [1.0, 0.0, -1.0], [0.0, 0.5, 0.5]])
    moments = np.kron(np.kron(powers, powers), powers)
    inverse = np.kron(np.kron(undo, undo), undo)
    return speeds, weights, moments, inverse


def relax_matrix(rates):
    speeds, weights, moments, inverse = lattice_tables()
    left_part = jnp.asarray(inverse / weights[:, None], jnp.float32) * rates[None, :]
    right_part = jnp.asarray(moments * weights[None, :], jnp.float32)
    return jnp.dot(left_part, right_part, precision=lax.Precision.HIGHEST)


def equilibrium(density, velocity):
    speeds = lattice_tables()[0]
    square = velocity[0] * velocity[0] + velocity[1] * velocity[1] + velocity[2] * velocity[2]
    columns = []
    for k in range(27):
        projected = float(speeds[k, 0]) * velocity[0] + float(speeds[k, 1]) * velocity[1] + float(speeds[k, 2]) * velocity[2]
        columns.append(density * (1.0 + 3.0 * projected + 4.5 * projected * projected - 1.5 * square))
    return jnp.stack(columns)


def macroscopic(scaled):
    speeds, weights, moments, inverse = lattice_tables()
    weight_vec = jnp.asarray(weights, jnp.float32)
    moment_rows = jnp.asarray((weights[:, None] * speeds).T, jnp.float32)
    density = jnp.tensordot(weight_vec, scaled, axes=1, precision=lax.Precision.HIGHEST)
    momentum = jnp.tensordot(moment_rows, scaled, axes=1, precision=lax.Precision.HIGHEST)
    return density, momentum / density[None]


def collide(scaled, matrix):
    density, velocity = macroscopic(scaled)
    layout = scaled.shape
    flattened = (scaled - equilibrium(density, velocity)).reshape(27, -1)
    return scaled - jnp.dot(matrix, flattened, precision=lax.Precision.HIGHEST).reshape(layout)


def profile_velocity(profile, vent_table):
    matches = (profile[None] == jnp.arange(vent_table.shape[0], dtype=jnp.int32)[:, None, None, None]).astype(vent_table.dtype)
    return jnp.tensordot(vent_table.T, matches, axes=1, precision=lax.Precision.HIGHEST)


def finish_pull(collided, shifted_x, types_pad, wall_pad, k):
    speeds = lattice_tables()[0]
    step_x, step_y, step_z = int(speeds[k, 0]), int(speeds[k, 1]), int(speeds[k, 2])
    width_x, width_y, width_z = collided.shape[1], collided.shape[2], collided.shape[3]
    padded = jnp.pad(shifted_x, ((0, 0), (1, 1), (1, 1)))
    source = padded[:, 1 - step_y:1 - step_y + width_y, 1 - step_z:1 - step_z + width_z]
    types_src = types_pad[1 - step_x:1 - step_x + width_x, 1 - step_y:1 - step_y + width_y, 1 - step_z:1 - step_z + width_z]
    wall_src = wall_pad[:, 1 - step_x:1 - step_x + width_x, 1 - step_y:1 - step_y + width_y, 1 - step_z:1 - step_z + width_z]
    projected = float(step_x) * wall_src[0] + float(step_y) * wall_src[1] + float(step_z) * wall_src[2]
    bounce = collided[26 - k] + jnp.where(types_src == 2, 6.0 * projected, 0.0)
    open_cell = (types_src == 0) | (types_src >= 3)
    return jnp.where(open_cell, source, bounce)


def apply_cells(passed, cell_types, cell_speed):
    density, velocity = macroscopic(passed)
    unity = jnp.ones_like(density)
    forced_in = equilibrium(unity, cell_speed)
    forced_out = equilibrium(unity, velocity)
    result = jnp.where(cell_types == 0, passed, 1.0)
    result = jnp.where(cell_types == 3, forced_in, result)
    return jnp.where(cell_types == 4, forced_out, result)


def to_room(blocked):
    blocked = jnp.roll(blocked, PY // 2, axis=blocked.ndim - 4)
    lead = blocked.shape[:-4]
    count, depth, rows, cells = blocked.shape[-4:]
    split = blocked.reshape(lead + (count // PY, PY, depth, rows, cells))
    split = jnp.swapaxes(split, -4, -3)
    return split.reshape(lead + ((count // PY) * depth, PY * rows, cells))


def to_blocks(room, depth, rows):
    lead = room.shape[:-3]
    cells = room.shape[-1]
    split = room.reshape(lead + (room.shape[-3] // depth, depth, PY, rows, cells))
    split = jnp.swapaxes(split, -4, -3)
    blocked = split.reshape(lead + ((room.shape[-3] // depth) * PY, depth, rows, cells))
    return jnp.roll(blocked, -(PY // 2), axis=blocked.ndim - 4)


def reference(populations, cell_kind, profile, vent_table, rates):
    depth, rows = populations.shape[2], populations.shape[3]
    speeds = lattice_tables()[0]
    matrix = relax_matrix(rates)
    room_kind = to_room(cell_kind)
    room_profile = to_room(profile)
    types_pad = jnp.pad(jnp.pad(room_kind, ((1, 1), (0, 0), (0, 0)), mode="wrap"), ((0, 0), (1, 1), (1, 1)), constant_values=1)
    profile_pad = jnp.pad(jnp.pad(room_profile, ((1, 1), (0, 0), (0, 0)), mode="wrap"), ((0, 0), (1, 1), (1, 1)))
    wall_pad = profile_velocity(profile_pad, vent_table)
    cell_speed = wall_pad[:, 1:-1, 1:-1, 1:-1]
    scaled = to_room(populations)
    for iteration in range(STEPS):
        collided = collide(scaled, matrix)
        pulled = []
        for k in range(27):
            shifted_x = jnp.roll(collided[k], int(speeds[k, 0]), axis=0)
            pulled.append(finish_pull(collided, shifted_x, types_pad, wall_pad, k))
        scaled = apply_cells(jnp.stack(pulled), room_kind, cell_speed)
    return to_blocks(scaled, depth, rows)
```

```python
import jax
import jax.numpy as jnp
from jax import lax
from jax.experimental import pallas as pl
from jax.experimental.pallas import tpu as pltpu
from jax.sharding import PartitionSpec as P

PY = 8
STEPS = 3
BIG = 1e30
MESH = pl.DeviceIdType.MESH

RIGHT, LEFT, UP, DOWN, RIGHT_UP, LEFT_DOWN, RIGHT_DOWN, LEFT_UP = range(8)
OFFSETS = (PY, -PY, 1, -1, PY + 1, -PY - 1, PY - 1, -PY + 1)


def direction(a, b, e):
    return 9 * (a + 1) + 3 * (b + 1) + (e + 1)


def digits(k):
    return (k // 9, k // 3 % 3, k % 3)


def forward(values):
    values = list(values)
    for stride in (1, 3, 9):
        for k in range(27):
            if k // stride % 3 == 0:
                low, mid, high = (values[k], values[k + stride], values[k + 2 * stride])
                both = low + high
                values[k] = both + 4.0 * mid
                values[k + stride] = high - low
                values[k + 2 * stride] = both
    return values


def backward(values):
    values = list(values)
    for stride in (9, 3, 1):
        for k in range(27):
            if k // stride % 3 == 0:
                zero, one, two = (values[k], values[k + stride], values[k + 2 * stride])
                values[k] = two - one
                values[k + stride] = zero - 0.5 * two
                values[k + 2 * stride] = two + one
    return values


def equilibrium_moments(density, velocity):
    share = [density]
    for _ in range(3):
        share.append(share[-1] * (1.0 / 3.0))
    triple = [3.0 * component * component for component in velocity]
    result = []
    for k in range(27):
        powers = digits(k)
        ones = [axis for axis in range(3) if powers[axis] == 1]
        twos = [axis for axis in range(3) if powers[axis] == 2]
        scale = share[len(twos)]
        if len(ones) == 0:
            shape = None
            for axis in twos:
                shape = 1.0 + triple[axis] if shape is None else shape + triple[axis]
            result.append(scale if shape is None else scale * shape)
        elif len(ones) == 3:
            result.append(None)
        else:
            shape = velocity[ones[0]]
            for axis in ones[1:]:
                shape = shape * velocity[axis]
            result.append(scale * shape)
    return result


def equilibrium(velocity):
    square = velocity[0] * velocity[0] + velocity[1] * velocity[1] + velocity[2] * velocity[2]
    base = 1.0 - 1.5 * square
    result = [None] * 27
    result[13] = base
    for k in range(13):
        projected = None
        for axis, digit in enumerate(digits(k)):
            if digit != 1:
                term = velocity[axis] if digit == 2 else -velocity[axis]
                projected = term if projected is None else projected + term
        even = base + 4.5 * projected * projected
        odd = 3.0 * projected
        result[k] = even + odd
        result[26 - k] = even - odd
    return result


def shifted(main, row, b, e, lane_count):
    if b != 0:
        count = main.shape[0]
        place = lax.broadcasted_iota(jnp.int32, main.shape, 0)
        moved = pltpu.roll(main, 1 if b == 1 else count - 1, 0)
        main = jnp.where(place == (0 if b == 1 else count - 1), row, moved)
    if e != 0:
        main = pltpu.roll(main, 1 if e == 1 else lane_count - 1, 1)
    return main


def kernel(
    populations, cell_kind, profile, vent_table, rates, out,
    start, collided, passed, walls, inlet, coef, kinds, profiles,
    rim_kinds, rim_profiles, fields, rim_fields,
    get_x, put_y, get_y, put_d, get_d,
    put_kx, get_kx, put_ky, get_ky, put_kd, get_kd,
    load_sem, out_sem, send_sem, recv_sem,
):
    me = lax.axis_index("gx")
    count = lax.axis_size("gx")
    depth, rows, cells = collided.shape[2], collided.shape[3], collided.shape[4]
    last = depth - 1
    half = cells // 2
    row_place = lax.rem(me + PY // 2, PY)
    targets = [lax.rem(me + count + offset, count) for offset in OFFSETS]

    barrier = pltpu.get_barrier_semaphore()
    for target in targets:
        pl.semaphore_signal(barrier, inc=1, device_id={"gx": target}, device_id_type=MESH)

    order = (0, last) + tuple(range(1, last))
    loads = {}
    for x in order:
        loads[x] = pltpu.make_async_copy(populations.at[:, 0, x], start.at[:, x], load_sem.at[x])
        loads[x].start()
    kind_load = pltpu.make_async_copy(cell_kind.at[0], kinds, load_sem.at[depth])
    profile_load = pltpu.make_async_copy(profile.at[0], profiles, load_sem.at[depth + 1])
    kind_load.start()
    profile_load.start()

    def remote(source, target_ref, slot, message):
        return pltpu.make_async_remote_copy(
            src_ref=source,
            dst_ref=target_ref,
            send_sem=send_sem.at[slot, message],
            recv_sem=recv_sem.at[slot, message],
            device_id={"gx": targets[message]},
            device_id_type=MESH,
        )

    def message(step, which):
        if which == RIGHT:
            return remote(collided.at[step, pl.ds(18, 9), last], get_x.at[step, 0], step, which)
        if which == LEFT:
            return remote(collided.at[step, pl.ds(0, 9), 0], get_x.at[step, 1], step, which)
        if which in (UP, DOWN):
            return remote(put_y.at[step, which - UP], get_y.at[step, which - UP], step, which)
        return remote(put_d.at[step, which - RIGHT_UP], get_d.at[step, which - RIGHT_UP], step, which)

    def kind_message(which):
        if which in (RIGHT, LEFT):
            return remote(put_kx.at[which], get_kx.at[which], STEPS, which)
        if which in (UP, DOWN):
            return remote(put_ky.at[which - UP], get_ky.at[which - UP], STEPS, which)
        return remote(put_kd.at[which - RIGHT_UP], get_kd.at[which - RIGHT_UP], STEPS, which)

    for k in range(27):
        scale = 1.0
        for digit in digits(k):
            scale = scale * (0.25 if digit == 0 else 0.5)
        rate = rates[k]
        coef[2 * k] = jnp.full((rows, half), scale * (1.0 - rate), jnp.float32)
        coef[2 * k + 1] = jnp.full((rows, half), scale * rate, jnp.float32)

    def relaxed(moments, target):
        result = []
        for k in range(27):
            value = coef[2 * k] * moments[k]
            if target[k] is not None:
                value = value + coef[2 * k + 1] * target[k]
            result.append(value)
        return backward(result)

    def collide_first(x, lanes):
        moments = forward([start[k, x, :, lanes] for k in range(27)])
        density = moments[0]
        velocity = [moments[k] / density for k in (9, 3, 1)]
        result = relaxed(moments, equilibrium_moments(density, velocity))
        for k in range(27):
            collided[0, k, x, :, lanes] = result[k]

    def cell_state(step, x, lanes):
        values = [
            collided[step, k, x, :, lanes] if k == 13 else passed[k, x, :, lanes]
            for k in range(27)
        ]
        moments = forward(values)
        velocity = [moments[k] / moments[0] for k in (9, 3, 1)]
        return (values, moments, velocity, kinds[x, :, lanes])

    def collide_next(step, x, lanes):
        values, moments, velocity, kind = cell_state(step, x, lanes)
        fluid = kind == 0
        moving = fluid | (kind == 4)
        velocity = [
            jnp.where(moving, velocity[axis], inlet[axis, x, :, lanes]) for axis in range(3)
        ]
        density = jnp.where(fluid, moments[0], 216.0)
        target = equilibrium_moments(density, velocity)
        moments = [
            jnp.where(fluid, moments[k], 0.0 if target[k] is None else target[k])
            for k in range(27)
        ]
        result = relaxed(moments, target)
        for k in range(27):
            collided[step + 1, k, x, :, lanes] = result[k]

    def finish(step, x, lanes):
        values, moments, velocity, kind = cell_state(step, x, lanes)
        fluid = kind == 0
        velocity = [
            jnp.where(kind == 4, velocity[axis], inlet[axis, x, :, lanes]) for axis in range(3)
        ]
        forced = equilibrium(velocity)
        for k in range(27):
            start[k, x, :, lanes] = jnp.where(fluid, values[k], forced[k])

    def by_halves(work, planes):
        def body(index, carry):
            plane = planes[0] + index // 2
            lanes = pl.ds(pl.multiple_of(index % 2 * half, half), half)
            work(plane, lanes)
            return carry

        lax.fori_loop(0, 2 * len(planes), body, 0)

    def stage_diagonal(step, which):
        a = 1 if which in (RIGHT_UP, RIGHT_DOWN) else -1
        b = 1 if which in (RIGHT_UP, LEFT_UP) else -1
        x = last if a == 1 else 0
        y = rows - 1 if b == 1 else 0
        for e in range(3):
            row = collided[step, direction(a, b, e - 1), x, pl.ds(y, 1), :]
            put_d[step, which - RIGHT_UP, pl.ds(2 * e, 1), :] = row[:, :half]
            put_d[step, which - RIGHT_UP, pl.ds(2 * e + 1, 1), :] = row[:, half:]

    def stage_rows(step):
        for which, b, y in ((0, 1, rows - 1), (1, -1, 0)):
            for pair in range(9):
                k = direction(pair // 3 - 1, b, pair % 3 - 1)
                for x in range(depth):
                    put_y[step, which, pl.ds(pair * depth + x, 1), :] = collided[
                        step, k, x, pl.ds(y, 1), :
                    ]

    def passed_plane(step, x):
        for k in range(27):
            if k == 13:
                continue
            a, b, e = (digit - 1 for digit in digits(k))
            origin = x - a
            row = None
            if origin < 0 or origin > last:
                side = 0 if a == 1 else 1
                main = get_x[step, side, 3 * (b + 1) + (e + 1)]
                if b != 0:
                    if a == 1:
                        which = RIGHT_UP if b == 1 else RIGHT_DOWN
                    else:
                        which = LEFT_UP if b == 1 else LEFT_DOWN
                    corner = get_d.at[step, which - RIGHT_UP]
                    row = jnp.concatenate(
                        [corner[pl.ds(2 * e + 2, 1), :], corner[pl.ds(2 * e + 3, 1), :]], axis=1
                    )
            else:
                main = collided[step, k, origin]
                if b != 0:
                    place = (3 * (a + 1) + (e + 1)) * depth + origin
                    row = get_y[step, 0 if b == 1 else 1, pl.ds(place, 1), :]
            source = shifted(main, row, b, e, cells)
            wall = walls[k, x]
            passed[k, x] = jnp.where(wall > 0.5 * BIG, source, collided[step, 26 - k, x] + wall)

    def field_values(kind, index):
        velocity = [jnp.zeros(kind.shape, jnp.float32) for _ in range(3)]
        for entry in range(vent_table.shape[0]):
            chosen = index == entry
            for axis in range(3):
                velocity[axis] = jnp.where(chosen, vent_table[entry, axis], velocity[axis])
        is_open = (kind == 0) | (kind >= 3)
        vent = kind == 2
        result = [jnp.where(is_open, BIG, 0.0)]
        for axis in range(3):
            result.append(jnp.where(vent, velocity[axis], 0.0))
        return result, velocity

    def prepare_walls():
        for plane in range(depth + 2):
            if plane == 0:
                kind, index = get_kx[RIGHT, 0], get_kx[RIGHT, 1]
            elif plane == depth + 1:
                kind, index = get_kx[LEFT, 0], get_kx[LEFT, 1]
            else:
                kind, index = kinds[plane - 1], profiles[plane - 1]
            values, velocity = field_values(kind, index)
            for field in range(4):
                fields[field, plane] = values[field]
            if 1 <= plane <= depth:
                for axis in range(3):
                    inlet[axis, plane - 1] = jnp.where(kind == 3, velocity[axis], 0.0)
        for side, b in ((0, 1), (1, -1)):
            low = (RIGHT_UP if b == 1 else RIGHT_DOWN) - RIGHT_UP
            high = (LEFT_UP if b == 1 else LEFT_DOWN) - RIGHT_UP
            for target, shift in ((rim_kinds, 0), (rim_profiles, 1)):
                target[side] = jnp.zeros((rows, cells), jnp.int32)
                target[side, pl.ds(1, depth), :] = get_ky[side, pl.ds(shift * depth, depth), :]
                for row, corner in ((0, low), (depth + 1, high)):
                    for part in range(2):
                        target[side, pl.ds(row, 1), pl.ds(part * half, half)] = get_kd[
                            corner, pl.ds(2 * shift + part, 1), :
                        ]
            outside = row_place == (0 if b == 1 else PY - 1)
            kind = jnp.where(outside, 1, rim_kinds[side])
            values, _ = field_values(kind, rim_profiles[side])
            for field in range(4):
                rim_fields[side, field] = values[field]
        lane = lax.broadcasted_iota(jnp.int32, (rows, cells), 1)
        for plane in range(depth + 2):
            for b in (-1, 0, 1):
                for e in (-1, 0, 1):
                    moved = []
                    for field in range(4):
                        row = None
                        if b != 0:
                            row = rim_fields[0 if b == 1 else 1, field, pl.ds(plane, 1), :]
                        value = shifted(fields[field, plane], row, b, e, cells)
                        if e != 0:
                            value = jnp.where(lane == (0 if e == 1 else cells - 1), 0.0, value)
                        moved.append(value)
                    cross = moved[0]
                    if b != 0:
                        cross = cross + (6.0 * b) * moved[2]
                    if e != 0:
                        cross = cross + (6.0 * e) * moved[3]
                    for a in (-1, 0, 1):
                        x = plane - 1 + a
                        k = direction(a, b, e)
                        if 0 <= x <= last and k != 13:
                            walls[k, x] = cross if a == 0 else cross + (6.0 * a) * moved[1]

    for x in order:
        loads[x].wait()
        by_halves(collide_first, (x,))
    for which in range(RIGHT_UP, LEFT_UP + 1):
        stage_diagonal(0, which)
    stage_rows(0)
    kind_load.wait()
    profile_load.wait()
    for which, x in ((RIGHT, last), (LEFT, 0)):
        put_kx[which, 0] = kinds[x]
        put_kx[which, 1] = profiles[x]
    for side, y in ((0, rows - 1), (1, 0)):
        for x in range(depth):
            put_ky[side, pl.ds(x, 1), :] = kinds[x, pl.ds(y, 1), :]
            put_ky[side, pl.ds(depth + x, 1), :] = profiles[x, pl.ds(y, 1), :]
    for which in range(RIGHT_UP, LEFT_UP + 1):
        x = last if which in (RIGHT_UP, RIGHT_DOWN) else 0
        y = rows - 1 if which in (RIGHT_UP, LEFT_UP) else 0
        for shift, source in ((0, kinds), (1, profiles)):
            row = source[x, pl.ds(y, 1), :]
            put_kd[which - RIGHT_UP, pl.ds(2 * shift, 1), :] = row[:, :half]
            put_kd[which - RIGHT_UP, pl.ds(2 * shift + 1, 1), :] = row[:, half:]

    pl.semaphore_wait(barrier, len(targets))
    for which in range(8):
        message(0, which).start()
    for which in range(8):
        kind_message(which).start()

    outs = []
    for step in range(STEPS):
        final = step == STEPS - 1
        work = finish if final else collide_next

        def advance(planes):
            for x in planes:
                passed_plane(step, x)
            by_halves(lambda x, lanes: work(step, x, lanes), planes)
            if final:
                for x in planes:
                    copy = pltpu.make_async_copy(start.at[:, x], out.at[:, 0, x], out_sem.at[x])
                    copy.start()
                    outs.append(copy)

        if step == 0:
            for which in range(8):
                kind_message(which).wait_recv()
            prepare_walls()
        for which in (UP, DOWN):
            message(step, which).wait_recv()
        advance(tuple(range(1, last)))
        for x, needed, sent in (
            (0, (RIGHT, RIGHT_UP, RIGHT_DOWN), (LEFT, LEFT_DOWN, LEFT_UP)),
            (last, (LEFT, LEFT_DOWN, LEFT_UP), (RIGHT, RIGHT_UP, RIGHT_DOWN)),
        ):
            for which in needed:
                message(step, which).wait_recv()
            advance((x,))
            if not final:
                message(step + 1, sent[0]).start()
                for which in sent[1:]:
                    stage_diagonal(step + 1, which)
                    message(step + 1, which).start()
        if not final:
            stage_rows(step + 1)
            for which in (UP, DOWN):
                message(step + 1, which).start()

    for step in range(STEPS):
        for which in range(8):
            message(step, which).wait_send()
    for which in range(8):
        kind_message(which).wait_send()
    for copy in outs:
        copy.wait()


def local(populations, cell_kind, profile, vent_table, rates):
    _, _, depth, rows, cells = populations.shape
    half = cells // 2
    strip = (9 * depth + 7) // 8 * 8
    f32, i32 = jnp.float32, jnp.int32
    anywhere = pl.BlockSpec(memory_space=pl.ANY)
    scalar = pl.BlockSpec(memory_space=pltpu.SMEM)
    return pl.pallas_call(
        kernel,
        out_shape=jax.ShapeDtypeStruct(populations.shape, f32),
        in_specs=[anywhere, anywhere, anywhere, scalar, scalar],
        out_specs=anywhere,
        scratch_shapes=[
            pltpu.VMEM((27, depth, rows, cells), f32),
            pltpu.VMEM((STEPS, 27, depth, rows, cells), f32),
            pltpu.VMEM((27, depth, rows, cells), f32),
            pltpu.VMEM((27, depth, rows, cells), f32),
            pltpu.VMEM((3, depth, rows, cells), f32),
            pltpu.VMEM((54, rows, half), f32),
            pltpu.VMEM((depth, rows, cells), i32),
            pltpu.VMEM((depth, rows, cells), i32),
            pltpu.VMEM((2, rows, cells), i32),
            pltpu.VMEM((2, rows, cells), i32),
            pltpu.VMEM((4, depth + 2, rows, cells), f32),
            pltpu.VMEM((2, 4, rows, cells), f32),
            pltpu.VMEM((STEPS, 2, 9, rows, cells), f32),
            pltpu.VMEM((STEPS, 2, strip, cells), f32),
            pltpu.VMEM((STEPS, 2, strip, cells), f32),
            pltpu.VMEM((STEPS, 4, 8, half), f32),
            pltpu.VMEM((STEPS, 4, 8, half), f32),
            pltpu.VMEM((2, 2, rows, cells), i32),
            pltpu.VMEM((2, 2, rows, cells), i32),
            pltpu.VMEM((2, 2 * depth, cells), i32),
            pltpu.VMEM((2, 2 * depth, cells), i32),
            pltpu.VMEM((4, 8, half), i32),
            pltpu.VMEM((4, 8, half), i32),
            pltpu.SemaphoreType.DMA((depth + 2,)),
            pltpu.SemaphoreType.DMA((depth,)),
            pltpu.SemaphoreType.DMA((STEPS + 1, 8)),
            pltpu.SemaphoreType.DMA((STEPS + 1, 8)),
        ],
        compiler_params=pltpu.CompilerParams(collective_id=0, has_side_effects=True),
        name="lattice_steps",
    )(populations, cell_kind, profile, vent_table, rates)


def solution(mesh):
    return jax.shard_map(
        local,
        mesh=mesh,
        in_specs=(
            P("scen", "gx", None, None, None),
            P("gx", None, None, "scen"),
            P("gx", None, None, "scen"),
            P("scen", None),
            P(),
        ),
        out_specs=P("scen", "gx", None, None, None),
        check_vma=False,
    )
```

```python
import jax
import jax.numpy as jnp
from jax import lax
from jax.experimental import pallas as pl
from jax.experimental.pallas import tpu as pltpu
from jax.sharding import PartitionSpec as P

PY = 8
STEPS = 3
BIG = 1e30
MESH = pl.DeviceIdType.MESH

ACROSS, CORNER, ALONG, ROW = 0, 2, 6, 12


def direction(a, b, e):
    return 9 * (a + 1) + 3 * (b + 1) + (e + 1)


def digits(k):
    return (k // 9, k // 3 % 3, k % 3)


def forward(values):
    values = list(values)
    for stride in (1, 3, 9):
        for k in range(27):
            if k // stride % 3 == 0:
                low, mid, high = (values[k], values[k + stride], values[k + 2 * stride])
                both = low + high
                values[k] = both + 4.0 * mid
                values[k + stride] = high - low
                values[k + 2 * stride] = both
    return values


def backward(values):
    values = list(values)
    for stride in (9, 3, 1):
        for k in range(27):
            if k // stride % 3 == 0:
                zero, one, two = (values[k], values[k + stride], values[k + 2 * stride])
                values[k] = two - one
                values[k + stride] = zero - 0.5 * two
                values[k + 2 * stride] = two + one
    return values


def equilibrium_moments(density, velocity):
    share = [density]
    for _ in range(3):
        share.append(share[-1] * (1.0 / 3.0))
    triple = [3.0 * component * component for component in velocity]
    result = []
    for k in range(27):
        powers = digits(k)
        ones = [axis for axis in range(3) if powers[axis] == 1]
        twos = [axis for axis in range(3) if powers[axis] == 2]
        scale = share[len(twos)]
        if len(ones) == 0:
            shape = None
            for axis in twos:
                shape = 1.0 + triple[axis] if shape is None else shape + triple[axis]
            result.append(scale if shape is None else scale * shape)
        elif len(ones) == 3:
            result.append(None)
        else:
            shape = velocity[ones[0]]
            for axis in ones[1:]:
                shape = shape * velocity[axis]
            result.append(scale * shape)
    return result


def equilibrium(velocity):
    square = velocity[0] * velocity[0] + velocity[1] * velocity[1] + velocity[2] * velocity[2]
    base = 1.0 - 1.5 * square
    result = [None] * 27
    result[13] = base
    for k in range(13):
        projected = None
        for axis, digit in enumerate(digits(k)):
            if digit != 1:
                term = velocity[axis] if digit == 2 else -velocity[axis]
                projected = term if projected is None else projected + term
        even = base + 4.5 * projected * projected
        odd = 3.0 * projected
        result[k] = even + odd
        result[26 - k] = even - odd
    return result


def shifted(main, row, b, e, lane_count):
    if b != 0:
        count = main.shape[0]
        place = lax.broadcasted_iota(jnp.int32, main.shape, 0)
        moved = pltpu.roll(main, 1 if b == 1 else count - 1, 0)
        main = jnp.where(place == (0 if b == 1 else count - 1), row, moved)
    if e != 0:
        main = pltpu.roll(main, 1 if e == 1 else lane_count - 1, 1)
    return main


def kernel(
    populations, cell_kind, profile, vent_table, rates, out,
    start, collided, passed, walls, inlet, coef, kinds, profiles,
    rim_kinds, rim_profiles, fields, rim_fields,
    get_x, put_y, get_y, put_d, get_d,
    put_kx, get_kx, put_ky, get_ky, put_kd, get_kd,
    load_sem, out_sem, send_sem, recv_sem,
):
    me = lax.axis_index("gx")
    count = lax.axis_size("gx")
    depth, rows, cells = collided.shape[2], collided.shape[3], collided.shape[4]
    last = depth - 1
    half = cells // 2
    row_place = lax.rem(me + PY // 2, PY)
    far_right = lax.rem(me // PY, 2) == 1
    has_row = (row_place != PY - 1, row_place != 0)

    def device(side, turn):
        place = me + count
        if side is not None:
            place = place + (PY - 2 * PY * side)
        if turn is not None:
            place = place + (1 - 2 * turn)
        return lax.rem(place, count)

    barrier = pltpu.get_barrier_semaphore()
    for side in (None, 0, 1):
        for turn in (None, 0, 1):
            if side is not None or turn is not None:
                pl.semaphore_signal(
                    barrier, inc=1, device_id={"gx": device(side, turn)}, device_id_type=MESH
                )

    order = (0, last) + tuple(range(1, last))
    loads = {}
    for x in order:
        loads[x] = pltpu.make_async_copy(populations.at[:, 0, x], start.at[:, x], load_sem.at[x])
        loads[x].start()
    kind_load = pltpu.make_async_copy(cell_kind.at[0], kinds, load_sem.at[depth])
    profile_load = pltpu.make_async_copy(profile.at[0], profiles, load_sem.at[depth + 1])
    kind_load.start()
    profile_load.start()

    def remote(source, target_ref, slot, place, side, turn):
        return pltpu.make_async_remote_copy(
            src_ref=source,
            dst_ref=target_ref,
            send_sem=send_sem.at[slot, place],
            recv_sem=recv_sem.at[slot, place],
            device_id={"gx": device(side, turn)},
            device_id_type=MESH,
        )

    def across(step, side):
        source = collided.at[step, pl.ds(18 - 18 * side, 9), last - last * side]
        return remote(source, get_x.at[step, side], step, ACROSS + side, side, None)

    def corner(step, side, turn):
        place = 2 * side + turn
        return remote(
            put_d.at[step, place], get_d.at[step, place], step, CORNER + place, side, turn
        )

    def along(step, turn, first, size, place):
        part = pl.ds(first, size)
        return remote(
            put_y.at[step, turn, part], get_y.at[step, turn, part], step,
            ALONG + 3 * turn + place, None, turn,
        )

    def along_edge(step, turn, side):
        return along(step, turn, 9 * last - (9 * last - 3) * side, 6, 2 - 2 * side)

    def along_middle(step, turn):
        return along(step, turn, 9, 9 * (last - 1), 1)

    def kind_across(side):
        return remote(put_kx.at[side], get_kx.at[side], STEPS, ACROSS + side, side, None)

    def kind_corner(side, turn):
        place = 2 * side + turn
        return remote(
            put_kd.at[place], get_kd.at[place], STEPS, CORNER + place, side, turn
        )

    def kind_along(turn):
        return remote(put_ky.at[turn], get_ky.at[turn], STEPS, ALONG + turn, None, turn)

    def go(copy, turn):
        @pl.when(has_row[turn])
        def _():
            copy().start()

    def sent(copy, turn):
        @pl.when(has_row[turn])
        def _():
            copy().wait_send()

    def came(copy, turn):
        @pl.when(has_row[1 - turn])
        def _():
            copy().wait_recv()

    for k in range(27):
        scale = 1.0
        for digit in digits(k):
            scale = scale * (0.25 if digit == 0 else 0.5)
        rate = rates[k]
        coef[2 * k] = jnp.full((rows, half), scale * (1.0 - rate), jnp.float32)
        coef[2 * k + 1] = jnp.full((rows, half), scale * rate, jnp.float32)

    def relaxed(moments, target):
        result = []
        for k in range(27):
            value = coef[2 * k] * moments[k]
            if target[k] is not None:
                value = value + coef[2 * k + 1] * target[k]
            result.append(value)
        return backward(result)

    def collide_first(x, lanes):
        moments = forward([start[k, x, :, lanes] for k in range(27)])
        density = moments[0]
        velocity = [moments[k] / density for k in (9, 3, 1)]
        result = relaxed(moments, equilibrium_moments(density, velocity))
        for k in range(27):
            collided[0, k, x, :, lanes] = result[k]

    def cell_state(step, x, lanes):
        values = [
            collided[step, k, x, :, lanes] if k == 13 else passed[k, x, :, lanes]
            for k in range(27)
        ]
        moments = forward(values)
        velocity = [moments[k] / moments[0] for k in (9, 3, 1)]
        return (values, moments, velocity, kinds[x, :, lanes])

    def collide_next(step, x, lanes):
        values, moments, velocity, kind = cell_state(step, x, lanes)
        fluid = kind == 0
        moving = fluid | (kind == 4)
        velocity = [
            jnp.where(moving, velocity[axis], inlet[axis, x, :, lanes]) for axis in range(3)
        ]
        density = jnp.where(fluid, moments[0], 216.0)
        target = equilibrium_moments(density, velocity)
        moments = [
            jnp.where(fluid, moments[k], 0.0 if target[k] is None else target[k])
            for k in range(27)
        ]
        result = relaxed(moments, target)
        for k in range(27):
            collided[step + 1, k, x, :, lanes] = result[k]

    def finish(step, x, lanes):
        values, moments, velocity, kind = cell_state(step, x, lanes)
        fluid = kind == 0
        velocity = [
            jnp.where(kind == 4, velocity[axis], inlet[axis, x, :, lanes]) for axis in range(3)
        ]
        forced = equilibrium(velocity)
        for k in range(27):
            start[k, x, :, lanes] = jnp.where(fluid, values[k], forced[k])

    def by_halves(work, first, planes):
        def body(index, carry):
            plane = first + index // 2
            lanes = pl.ds(pl.multiple_of(index % 2 * half, half), half)
            work(plane, lanes)
            return carry

        lax.fori_loop(0, 2 * planes, body, 0)

    def stage_corners(step, side):
        x = last - last * side
        for turn in range(2):
            y = rows - 1 if turn == 0 else 0
            for e in range(3):
                k = 18 - 18 * side + (6 - 6 * turn) + e
                put_d[step, 2 * side + turn, e] = collided[step, k, x, pl.ds(y, 1), :]

    def stage_rows(step, x, pairs):
        for turn in range(2):
            y = rows - 1 if turn == 0 else 0
            for pair in pairs:
                k = 9 * (pair // 3) + (6 - 6 * turn) + pair % 3
                put_y[step, turn, 9 * x + pair] = collided[step, k, x, pl.ds(y, 1), :]

    def stage_edge(step, side):
        x = last - last * side
        for turn in range(2):
            y = rows - 1 if turn == 0 else 0
            for pair in range(6):
                k = 9 * (pair // 3) + 9 * side + (6 - 6 * turn) + pair % 3
                row = 9 * last - (9 * last - 3) * side + pair
                put_y[step, turn, row] = collided[step, k, x, pl.ds(y, 1), :]

    def passed_on(step, k, x, opposite, main, row, b, e):
        source = shifted(main, row, b, e, cells)
        wall = walls[k, x]
        passed[k, x] = jnp.where(wall > 0.5 * BIG, source, collided[step, opposite, x] + wall)

    def passed_middle(step, x):
        for k in range(27):
            if k == 13:
                continue
            a, b, e = (digit - 1 for digit in digits(k))
            row = None
            if b != 0:
                row = get_y[step, (1 - b) // 2, 9 * (x - a) + 3 * (a + 1) + (e + 1)]
            passed_on(step, k, x, 26 - k, collided[step, k, x - a], row, b, e)

    def passed_edge(step, side):
        x = last * side
        into, back = (18 - 18 * side, 18 * side)
        inner = x + 1 - 2 * side
        for b in (-1, 0, 1):
            turn = (1 - b) // 2
            for e in (-1, 0, 1):
                place = 3 * (b + 1) + (e + 1)
                row = None
                if b != 0:
                    row = get_d[step, 2 * side + turn, e + 1]
                passed_on(
                    step, into + place, x, back + (8 - place), get_x[step, side, place], row, b, e
                )
                if b != 0 or e != 0:
                    if b != 0:
                        row = get_y[step, turn, 9 * x + 3 + (e + 1)]
                    passed_on(
                        step, 9 + place, x, 17 - place, collided[step, 9 + place, x], row, b, e
                    )
                if b != 0:
                    row = get_y[step, turn, 9 * inner + 6 * side + (e + 1)]
                passed_on(
                    step, back + place, x, into + (8 - place),
                    collided[step, back + place, inner], row, b, e,
                )

    def field_values(kind, index):
        velocity = [jnp.zeros(kind.shape, jnp.float32) for _ in range(3)]
        for entry in range(vent_table.shape[1]):
            chosen = index == entry
            for axis in range(3):
                velocity[axis] = jnp.where(chosen, vent_table[axis, entry], velocity[axis])
        is_open = (kind == 0) | (kind >= 3)
        vent = kind == 2
        result = [jnp.where(is_open, BIG, 0.0)]
        for axis in range(3):
            result.append(jnp.where(vent, velocity[axis], 0.0))
        return result, velocity

    def prepare_walls():
        for plane in range(depth + 2):
            if plane == 0:
                kind, index = get_kx[0, 0], get_kx[0, 1]
            elif plane == depth + 1:
                kind, index = get_kx[1, 0], get_kx[1, 1]
            else:
                kind, index = kinds[plane - 1], profiles[plane - 1]
            values, velocity = field_values(kind, index)
            for field in range(4):
                fields[field, plane] = values[field]
            if 1 <= plane <= depth:
                for axis in range(3):
                    inlet[axis, plane - 1] = jnp.where(kind == 3, velocity[axis], 0.0)
        for side in range(2):
            for target, shift in ((rim_kinds, 0), (rim_profiles, 1)):
                target[side] = jnp.zeros((rows, cells), jnp.int32)
                for x in range(depth):
                    target[side, pl.ds(x + 1, 1), :] = get_ky[side, shift * depth + x]
                for row, place in ((0, side), (depth + 1, 2 + side)):
                    target[side, pl.ds(row, 1), :] = get_kd[place, shift]
            outside = row_place == (0 if side == 0 else PY - 1)
            kind = jnp.where(outside, 1, rim_kinds[side])
            values, _ = field_values(kind, rim_profiles[side])
            for field in range(4):
                rim_fields[side, field] = values[field]
        lane = lax.broadcasted_iota(jnp.int32, (rows, cells), 1)
        for plane in range(depth + 2):
            for b in (-1, 0, 1):
                for e in (-1, 0, 1):
                    moved = []
                    for field in range(4):
                        row = None
                        if b != 0:
                            row = rim_fields[0 if b == 1 else 1, field, pl.ds(plane, 1), :]
                        value = shifted(fields[field, plane], row, b, e, cells)
                        if e != 0:
                            value = jnp.where(lane == (0 if e == 1 else cells - 1), 0.0, value)
                        moved.append(value)
                    cross = moved[0]
                    if b != 0:
                        cross = cross + (6.0 * b) * moved[2]
                    if e != 0:
                        cross = cross + (6.0 * e) * moved[3]
                    for a in (-1, 0, 1):
                        x = plane - 1 + a
                        k = direction(a, b, e)
                        if 0 <= x <= last and k != 13:
                            walls[k, x] = cross if a == 0 else cross + (6.0 * a) * moved[1]

    for x in order:
        loads[x].wait()
        by_halves(collide_first, x, 1)
    for side in range(2):
        stage_corners(0, side)
        stage_edge(0, side)
    for x in range(1, last):
        stage_rows(0, x, range(9))
    kind_load.wait()
    profile_load.wait()
    for side, x in ((0, last), (1, 0)):
        put_kx[side, 0] = kinds[x]
        put_kx[side, 1] = profiles[x]
        for turn in range(2):
            y = rows - 1 if turn == 0 else 0
            put_kd[2 * side + turn, 0] = kinds[x, pl.ds(y, 1), :]
            put_kd[2 * side + turn, 1] = profiles[x, pl.ds(y, 1), :]
    for turn in range(2):
        y = rows - 1 if turn == 0 else 0
        for x in range(depth):
            put_ky[turn, x] = kinds[x, pl.ds(y, 1), :]
            put_ky[turn, depth + x] = profiles[x, pl.ds(y, 1), :]

    far = jnp.where(far_right, 0, 1)
    sides = (far, 1 - far)
    pl.semaphore_wait(barrier, 8)
    for number, side in enumerate(sides):
        if number == 1:
            across(0, sides[0]).wait_send()
        across(0, side).start()
        for turn in range(2):
            go(lambda: corner(0, side, turn), turn)
        kind_across(side).start()
        for turn in range(2):
            go(lambda: kind_corner(side, turn), turn)
        if number == 0:
            for turn in range(2):
                go(lambda: along_middle(0, turn), turn)
                go(lambda: along_edge(0, turn, 0), turn)
                go(lambda: along_edge(0, turn, 1), turn)
                go(lambda: kind_along(turn), turn)

    outs = []
    for step in range(STEPS):
        final = step == STEPS - 1
        work = finish if final else collide_next

        def write(x, number):
            copy = pltpu.make_async_copy(start.at[:, x], out.at[:, 0, x], out_sem.at[number])
            copy.start()
            outs.append(copy)

        if step == 0:
            for side in range(2):
                kind_across(side).wait_recv()
                for turn in range(2):
                    came(lambda: kind_corner(side, turn), turn)
            for turn in range(2):
                came(lambda: kind_along(turn), turn)
            prepare_walls()
        for turn in range(2):
            came(lambda: along_middle(step, turn), turn)
            for side in range(2):
                came(lambda: along_edge(step, turn, side), turn)
        for x in range(1, last):
            passed_middle(step, x)
        by_halves(lambda x, lanes: work(step, x, lanes), 1, last - 1)
        if final:
            for x in range(1, last):
                write(x, x)
        else:
            for x in range(1, last):
                stage_rows(step + 1, x, range(9))
            for turn in range(2):
                go(lambda: along_middle(step + 1, turn), turn)
        for number, side in enumerate(sides):
            across(step, 1 - side).wait_recv()
            for turn in range(2):
                came(lambda: corner(step, 1 - side, turn), turn)
            passed_edge(step, 1 - side)
            x = last - last * side
            by_halves(lambda x, lanes: work(step, x, lanes), x, 1)
            if final:
                write(x, last * number)
            else:
                across(step + 1, side).start()
                stage_corners(step + 1, side)
                for turn in range(2):
                    go(lambda: corner(step + 1, side, turn), turn)
                stage_edge(step + 1, side)
                for turn in range(2):
                    go(lambda: along_edge(step + 1, turn, side), turn)

    for step in range(STEPS):
        for number, side in enumerate(sides):
            if step > 0 or number == 1:
                across(step, side).wait_send()
            for turn in range(2):
                sent(lambda: corner(step, side, turn), turn)
                sent(lambda: along_edge(step, turn, side), turn)
        for turn in range(2):
            sent(lambda: along_middle(step, turn), turn)
    for side in range(2):
        kind_across(side).wait_send()
        for turn in range(2):
            sent(lambda: kind_corner(side, turn), turn)
    for turn in range(2):
        sent(lambda: kind_along(turn), turn)
    for copy in outs:
        copy.wait()


def local(populations, cell_kind, profile, vent_table, rates):
    _, _, depth, rows, cells = populations.shape
    half = cells // 2
    strip = 9 * depth
    f32, i32 = jnp.float32, jnp.int32
    anywhere = pl.BlockSpec(memory_space=pl.ANY)
    scalar = pl.BlockSpec(memory_space=pltpu.SMEM)
    return pl.pallas_call(
        kernel,
        out_shape=jax.ShapeDtypeStruct(populations.shape, f32),
        in_specs=[anywhere, anywhere, anywhere, scalar, scalar],
        out_specs=anywhere,
        scratch_shapes=[
            pltpu.VMEM((27, depth, rows, cells), f32),
            pltpu.VMEM((STEPS, 27, depth, rows, cells), f32),
            pltpu.VMEM((27, depth, rows, cells), f32),
            pltpu.VMEM((27, depth, rows, cells), f32),
            pltpu.VMEM((3, depth, rows, cells), f32),
            pltpu.VMEM((54, rows, half), f32),
            pltpu.VMEM((depth, rows, cells), i32),
            pltpu.VMEM((depth, rows, cells), i32),
            pltpu.VMEM((2, rows, cells), i32),
            pltpu.VMEM((2, rows, cells), i32),
            pltpu.VMEM((4, depth + 2, rows, cells), f32),
            pltpu.VMEM((2, 4, rows, cells), f32),
            pltpu.VMEM((STEPS, 2, 9, rows, cells), f32),
            pltpu.VMEM((STEPS, 2, strip, 1, cells), f32),
            pltpu.VMEM((STEPS, 2, strip, 1, cells), f32),
            pltpu.VMEM((STEPS, 4, 3, 1, cells), f32),
            pltpu.VMEM((STEPS, 4, 3, 1, cells), f32),
            pltpu.VMEM((2, 2, rows, cells), i32),
            pltpu.VMEM((2, 2, rows, cells), i32),
            pltpu.VMEM((2, 2 * depth, 1, cells), i32),
            pltpu.VMEM((2, 2 * depth, 1, cells), i32),
            pltpu.VMEM((4, 2, 1, cells), i32),
            pltpu.VMEM((4, 2, 1, cells), i32),
            pltpu.SemaphoreType.DMA((depth + 2,)),
            pltpu.SemaphoreType.DMA((depth,)),
            pltpu.SemaphoreType.DMA((STEPS + 1, ROW)),
            pltpu.SemaphoreType.DMA((STEPS + 1, ROW)),
        ],
        compiler_params=pltpu.CompilerParams(collective_id=0, has_side_effects=True),
        name="lattice_steps",
    )(populations, cell_kind, profile, vent_table.T, rates)


def solution(mesh):
    return jax.shard_map(
        local,
        mesh=mesh,
        in_specs=(
            P("scen", "gx", None, None, None),
            P("gx", None, None, "scen"),
            P("gx", None, None, "scen"),
            P("scen", None),
            P(),
        ),
        out_specs=P("scen", "gx", None, None, None),
        check_vma=False,
    )
```

```python
import jax
import jax.numpy as jnp
from jax import lax
from jax.experimental import pallas as pl
from jax.experimental.pallas import tpu as pltpu
from jax.sharding import PartitionSpec as P

PY = 8
STEPS = 3
BIG = 1e30
MESH = pl.DeviceIdType.MESH

ACROSS, CORNER, ALONG, ROW = 0, 2, 6, 12


def direction(a, b, e):
    return 9 * (a + 1) + 3 * (b + 1) + (e + 1)


def digits(k):
    return (k // 9, k // 3 % 3, k % 3)


def forward(values):
    values = list(values)
    for stride in (1, 3, 9):
        for k in range(27):
            if k // stride % 3 == 0:
                low, mid, high = (values[k], values[k + stride], values[k + 2 * stride])
                both = low + high
                values[k] = both + 4.0 * mid
                values[k + stride] = high - low
                values[k + 2 * stride] = both
    return values


def backward(values):
    values = list(values)
    for stride in (9, 3, 1):
        for k in range(27):
            if k // stride % 3 == 0:
                zero, one, two = (values[k], values[k + stride], values[k + 2 * stride])
                values[k] = two - one
                values[k + stride] = zero - 0.5 * two
                values[k + 2 * stride] = two + one
    return values


def equilibrium_moments(density, velocity):
    share = [density]
    for _ in range(3):
        share.append(share[-1] * (1.0 / 3.0))
    triple = [3.0 * component * component for component in velocity]
    result = []
    for k in range(27):
        powers = digits(k)
        ones = [axis for axis in range(3) if powers[axis] == 1]
        twos = [axis for axis in range(3) if powers[axis] == 2]
        scale = share[len(twos)]
        if len(ones) == 0:
            shape = None
            for axis in twos:
                shape = 1.0 + triple[axis] if shape is None else shape + triple[axis]
            result.append(scale if shape is None else scale * shape)
        elif len(ones) == 3:
            result.append(None)
        else:
            shape = velocity[ones[0]]
            for axis in ones[1:]:
                shape = shape * velocity[axis]
            result.append(scale * shape)
    return result


def equilibrium(velocity):
    square = velocity[0] * velocity[0] + velocity[1] * velocity[1] + velocity[2] * velocity[2]
    base = 1.0 - 1.5 * square
    result = [None] * 27
    result[13] = base
    for k in range(13):
        projected = None
        for axis, digit in enumerate(digits(k)):
            if digit != 1:
                term = velocity[axis] if digit == 2 else -velocity[axis]
                projected = term if projected is None else projected + term
        even = base + 4.5 * projected * projected
        odd = 3.0 * projected
        result[k] = even + odd
        result[26 - k] = even - odd
    return result


def shifted(main, row, b, e, lane_count):
    if b != 0:
        count = main.shape[0]
        place = lax.broadcasted_iota(jnp.int32, main.shape, 0)
        moved = pltpu.roll(main, 1 if b == 1 else count - 1, 0)
        main = jnp.where(place == (0 if b == 1 else count - 1), row, moved)
    if e != 0:
        main = pltpu.roll(main, 1 if e == 1 else lane_count - 1, 1)
    return main


def kernel(
    populations, cell_kind, profile, vent_table, rates, out,
    start, collided, passed, walls, inlet, coef, kinds, profiles,
    rim_kinds, rim_profiles, fields, rim_fields,
    get_x, put_y, get_y, put_d, get_d,
    put_kx, get_kx, put_ky, get_ky, put_kd, get_kd,
    load_sem, out_sem, send_sem, recv_sem,
):
    me = lax.axis_index("gx")
    count = lax.axis_size("gx")
    depth, rows, cells = collided.shape[2], collided.shape[3], collided.shape[4]
    last = depth - 1
    half = cells // 2
    row_place = lax.rem(me + PY // 2, PY)
    far_right = lax.rem(me // PY, 2) == 1
    has_row = (row_place != PY - 1, row_place != 0)

    def device(side, turn):
        place = me + count
        if side is not None:
            place = place + (PY - 2 * PY * side)
        if turn is not None:
            place = place + (1 - 2 * turn)
        return lax.rem(place, count)

    barrier = pltpu.get_barrier_semaphore()
    for side in (None, 0, 1):
        for turn in (None, 0, 1):
            if side is not None or turn is not None:
                pl.semaphore_signal(
                    barrier, inc=1, device_id={"gx": device(side, turn)}, device_id_type=MESH
                )

    order = (0, last) + tuple(range(1, last))
    loads = {}
    for x in order:
        loads[x] = pltpu.make_async_copy(populations.at[:, 0, x], start.at[:, x], load_sem.at[x])
        loads[x].start()
    kind_load = pltpu.make_async_copy(cell_kind.at[0], kinds, load_sem.at[depth])
    profile_load = pltpu.make_async_copy(profile.at[0], profiles, load_sem.at[depth + 1])
    kind_load.start()
    profile_load.start()

    def remote(source, target_ref, slot, place, side, turn):
        return pltpu.make_async_remote_copy(
            src_ref=source,
            dst_ref=target_ref,
            send_sem=send_sem.at[slot, place],
            recv_sem=recv_sem.at[slot, place],
            device_id={"gx": device(side, turn)},
            device_id_type=MESH,
        )

    def across(step, side):
        source = collided.at[step, pl.ds(18 - 18 * side, 9), last - last * side]
        return remote(source, get_x.at[step, side], step, ACROSS + side, side, None)

    def corner(step, side, turn):
        place = 2 * side + turn
        return remote(
            put_d.at[step, place], get_d.at[step, place], step, CORNER + place, side, turn
        )

    def along(step, turn, first, size, place):
        part = pl.ds(first, size)
        return remote(
            put_y.at[step, turn, part], get_y.at[step, turn, part], step,
            ALONG + 3 * turn + place, None, turn,
        )

    def along_edge(step, turn, side):
        return along(step, turn, 9 * last - (9 * last - 3) * side, 6, 2 - 2 * side)

    def along_middle(step, turn):
        return along(step, turn, 9, 9 * (last - 1), 1)

    def kind_across(side):
        return remote(put_kx.at[side], get_kx.at[side], STEPS, ACROSS + side, side, None)

    def kind_corner(side, turn):
        place = 2 * side + turn
        return remote(
            put_kd.at[place], get_kd.at[place], STEPS, CORNER + place, side, turn
        )

    def kind_along(turn):
        return remote(put_ky.at[turn], get_ky.at[turn], STEPS, ALONG + turn, None, turn)

    def go(copy, turn):
        @pl.when(has_row[turn])
        def _():
            copy().start()

    def sent(copy, turn):
        @pl.when(has_row[turn])
        def _():
            copy().wait_send()

    def came(copy, turn):
        @pl.when(has_row[1 - turn])
        def _():
            copy().wait_recv()

    for k in range(27):
        scale = 1.0
        for digit in digits(k):
            scale = scale * (0.25 if digit == 0 else 0.5)
        rate = rates[k]
        coef[2 * k] = jnp.full((rows, half), scale * (1.0 - rate), jnp.float32)
        coef[2 * k + 1] = jnp.full((rows, half), scale * rate, jnp.float32)

    def relaxed(moments, target):
        result = []
        for k in range(27):
            value = coef[2 * k] * moments[k]
            if target[k] is not None:
                value = value + coef[2 * k + 1] * target[k]
            result.append(value)
        return backward(result)

    def collide_first(x, lanes):
        moments = forward([start[k, x, :, lanes] for k in range(27)])
        density = moments[0]
        velocity = [moments[k] / density for k in (9, 3, 1)]
        result = relaxed(moments, equilibrium_moments(density, velocity))
        for k in range(27):
            collided[0, k, x, :, lanes] = result[k]

    def cell_state(step, x, lanes):
        values = [
            collided[step, k, x, :, lanes] if k == 13 else passed[k, x, :, lanes]
            for k in range(27)
        ]
        moments = forward(values)
        velocity = [moments[k] / moments[0] for k in (9, 3, 1)]
        return (values, moments, velocity, kinds[x, :, lanes])

    def collide_next(step, x, lanes):
        values, moments, velocity, kind = cell_state(step, x, lanes)
        fluid = kind == 0
        moving = fluid | (kind == 4)
        velocity = [
            jnp.where(moving, velocity[axis], inlet[axis, x, :, lanes]) for axis in range(3)
        ]
        density = jnp.where(fluid, moments[0], 216.0)
        target = equilibrium_moments(density, velocity)
        moments = [
            jnp.where(fluid, moments[k], 0.0 if target[k] is None else target[k])
            for k in range(27)
        ]
        result = relaxed(moments, target)
        for k in range(27):
            collided[step + 1, k, x, :, lanes] = result[k]

    def finish(step, x, lanes):
        values, moments, velocity, kind = cell_state(step, x, lanes)
        fluid = kind == 0
        velocity = [
            jnp.where(kind == 4, velocity[axis], inlet[axis, x, :, lanes]) for axis in range(3)
        ]
        forced = equilibrium(velocity)
        for k in range(27):
            start[k, x, :, lanes] = jnp.where(fluid, values[k], forced[k])

    def by_halves(work, first, planes):
        def body(index, carry):
            plane = first + index // 2
            lanes = pl.ds(pl.multiple_of(index % 2 * half, half), half)
            work(plane, lanes)
            return carry

        lax.fori_loop(0, 2 * planes, body, 0)

    def stage_corners(step, side):
        x = last - last * side
        for turn in range(2):
            y = rows - 1 if turn == 0 else 0
            for e in range(3):
                k = 18 - 18 * side + (6 - 6 * turn) + e
                put_d[step, 2 * side + turn, e] = collided[step, k, x, pl.ds(y, 1), :]

    def stage_rows(step, x, pairs):
        for turn in range(2):
            y = rows - 1 if turn == 0 else 0
            for pair in pairs:
                k = 9 * (pair // 3) + (6 - 6 * turn) + pair % 3
                put_y[step, turn, 9 * x + pair] = collided[step, k, x, pl.ds(y, 1), :]

    def stage_edge(step, side):
        x = last - last * side
        for turn in range(2):
            y = rows - 1 if turn == 0 else 0
            for pair in range(6):
                k = 9 * (pair // 3) + 9 * side + (6 - 6 * turn) + pair % 3
                row = 9 * last - (9 * last - 3) * side + pair
                put_y[step, turn, row] = collided[step, k, x, pl.ds(y, 1), :]

    def passed_on(step, k, x, opposite, main, row, b, e):
        source = shifted(main, row, b, e, cells)
        wall = walls[k, x]
        passed[k, x] = jnp.where(wall > 0.5 * BIG, source, collided[step, opposite, x] + wall)

    def passed_middle(step, x):
        for k in range(27):
            if k == 13:
                continue
            a, b, e = (digit - 1 for digit in digits(k))
            row = None
            if b != 0:
                row = get_y[step, (1 - b) // 2, 9 * (x - a) + 3 * (a + 1) + (e + 1)]
            passed_on(step, k, x, 26 - k, collided[step, k, x - a], row, b, e)

    def passed_edge(step, side):
        x = last * side
        into, back = (18 - 18 * side, 18 * side)
        inner = x + 1 - 2 * side
        for b in (-1, 0, 1):
            turn = (1 - b) // 2
            for e in (-1, 0, 1):
                place = 3 * (b + 1) + (e + 1)
                row = None
                if b != 0:
                    row = get_d[step, 2 * side + turn, e + 1]
                passed_on(
                    step, into + place, x, back + (8 - place), get_x[step, side, place], row, b, e
                )
                if b != 0 or e != 0:
                    if b != 0:
                        row = get_y[step, turn, 9 * x + 3 + (e + 1)]
                    passed_on(
                        step, 9 + place, x, 17 - place, collided[step, 9 + place, x], row, b, e
                    )
                if b != 0:
                    row = get_y[step, turn, 9 * inner + 6 * side + (e + 1)]
                passed_on(
                    step, back + place, x, into + (8 - place),
                    collided[step, back + place, inner], row, b, e,
                )

    def field_values(kind, index):
        velocity = [jnp.zeros(kind.shape, jnp.float32) for _ in range(3)]
        for entry in range(vent_table.shape[1]):
            chosen = index == entry
            for axis in range(3):
                velocity[axis] = jnp.where(chosen, vent_table[axis, entry], velocity[axis])
        is_open = (kind == 0) | (kind >= 3)
        vent = kind == 2
        result = [jnp.where(is_open, BIG, 0.0)]
        for axis in range(3):
            result.append(jnp.where(vent, velocity[axis], 0.0))
        return result, velocity

    def prepare_walls():
        for plane in range(depth + 2):
            if plane == 0:
                kind, index = get_kx[0, 0], get_kx[0, 1]
            elif plane == depth + 1:
                kind, index = get_kx[1, 0], get_kx[1, 1]
            else:
                kind, index = kinds[plane - 1], profiles[plane - 1]
            values, velocity = field_values(kind, index)
            for field in range(4):
                fields[field, plane] = values[field]
            if 1 <= plane <= depth:
                for axis in range(3):
                    inlet[axis, plane - 1] = jnp.where(kind == 3, velocity[axis], 0.0)
        for side in range(2):
            for target, shift in ((rim_kinds, 0), (rim_profiles, 1)):
                target[side] = jnp.zeros((rows, cells), jnp.int32)
                for x in range(depth):
                    target[side, pl.ds(x + 1, 1), :] = get_ky[side, shift * depth + x]
                for row, place in ((0, side), (depth + 1, 2 + side)):
                    target[side, pl.ds(row, 1), :] = get_kd[place, shift]
            outside = row_place == (0 if side == 0 else PY - 1)
            kind = jnp.where(outside, 1, rim_kinds[side])
            values, _ = field_values(kind, rim_profiles[side])
            for field in range(4):
                rim_fields[side, field] = values[field]
        lane = lax.broadcasted_iota(jnp.int32, (rows, cells), 1)
        for plane in range(depth + 2):
            for b in (-1, 0, 1):
                for e in (-1, 0, 1):
                    moved = []
                    for field in range(4):
                        row = None
                        if b != 0:
                            row = rim_fields[0 if b == 1 else 1, field, pl.ds(plane, 1), :]
                        value = shifted(fields[field, plane], row, b, e, cells)
                        if e != 0:
                            value = jnp.where(lane == (0 if e == 1 else cells - 1), 0.0, value)
                        moved.append(value)
                    cross = moved[0]
                    if b != 0:
                        cross = cross + (6.0 * b) * moved[2]
                    if e != 0:
                        cross = cross + (6.0 * e) * moved[3]
                    for a in (-1, 0, 1):
                        x = plane - 1 + a
                        k = direction(a, b, e)
                        if 0 <= x <= last and k != 13:
                            walls[k, x] = cross if a == 0 else cross + (6.0 * a) * moved[1]

    for x in order:
        loads[x].wait()
        by_halves(collide_first, x, 1)
    for side in range(2):
        stage_corners(0, side)
        stage_edge(0, side)
    for x in range(1, last):
        stage_rows(0, x, range(9))
    kind_load.wait()
    profile_load.wait()
    for side, x in ((0, last), (1, 0)):
        put_kx[side, 0] = kinds[x]
        put_kx[side, 1] = profiles[x]
        for turn in range(2):
            y = rows - 1 if turn == 0 else 0
            put_kd[2 * side + turn, 0] = kinds[x, pl.ds(y, 1), :]
            put_kd[2 * side + turn, 1] = profiles[x, pl.ds(y, 1), :]
    for turn in range(2):
        y = rows - 1 if turn == 0 else 0
        for x in range(depth):
            put_ky[turn, x] = kinds[x, pl.ds(y, 1), :]
            put_ky[turn, depth + x] = profiles[x, pl.ds(y, 1), :]

    far = jnp.where(far_right, 0, 1)
    sides = (far, 1 - far)
    pl.semaphore_wait(barrier, 8)
    for side in sides:
        kind_across(side).start()
        for turn in range(2):
            go(lambda: kind_corner(side, turn), turn)
    for turn in range(2):
        go(lambda: kind_along(turn), turn)
    for number, side in enumerate(sides):
        if number == 1:
            across(0, sides[0]).wait_send()
        for turn in range(2):
            go(lambda: corner(0, side, turn), turn)
        across(0, side).start()
        if number == 0:
            for turn in range(2):
                go(lambda: along_middle(0, turn), turn)
                go(lambda: along_edge(0, turn, sides[0]), turn)
                go(lambda: along_edge(0, turn, sides[1]), turn)

    for side in sides:
        kind_across(side).wait_recv()
        for turn in range(2):
            came(lambda: kind_corner(side, turn), turn)
    for turn in range(2):
        came(lambda: kind_along(turn), turn)
    prepare_walls()

    outs = []
    for step in range(STEPS):
        final = step == STEPS - 1
        work = finish if final else collide_next

        def write(x, number):
            copy = pltpu.make_async_copy(start.at[:, x], out.at[:, 0, x], out_sem.at[number])
            copy.start()
            outs.append(copy)

        def edge(number):
            side = sides[number]
            across(step, 1 - side).wait_recv()
            for turn in range(2):
                came(lambda: corner(step, 1 - side, turn), turn)
            passed_edge(step, 1 - side)
            x = last - last * side
            by_halves(lambda x, lanes: work(step, x, lanes), x, 1)
            if final:
                write(x, last * number)
            else:
                stage_corners(step + 1, side)
                for turn in range(2):
                    go(lambda: corner(step + 1, side, turn), turn)
                stage_edge(step + 1, side)
                for turn in range(2):
                    go(lambda: along_edge(step + 1, turn, side), turn)
                across(step + 1, side).start()

        for turn in range(2):
            came(lambda: along_middle(step, turn), turn)
            came(lambda: along_edge(step, turn, sides[0]), turn)
        edge(0)
        for turn in range(2):
            came(lambda: along_edge(step, turn, sides[1]), turn)
        for x in range(1, last):
            passed_middle(step, x)
        by_halves(lambda x, lanes: work(step, x, lanes), 1, last - 1)
        if final:
            for x in range(1, last):
                write(x, x)
        else:
            for x in range(1, last):
                stage_rows(step + 1, x, range(9))
            for turn in range(2):
                go(lambda: along_middle(step + 1, turn), turn)
        edge(1)

    for step in range(STEPS):
        for number, side in enumerate(sides):
            if step > 0 or number == 1:
                across(step, side).wait_send()
            for turn in range(2):
                sent(lambda: corner(step, side, turn), turn)
                sent(lambda: along_edge(step, turn, side), turn)
        for turn in range(2):
            sent(lambda: along_middle(step, turn), turn)
    for side in range(2):
        kind_across(side).wait_send()
        for turn in range(2):
            sent(lambda: kind_corner(side, turn), turn)
    for turn in range(2):
        sent(lambda: kind_along(turn), turn)
    for copy in outs:
        copy.wait()


def local(populations, cell_kind, profile, vent_table, rates):
    _, _, depth, rows, cells = populations.shape
    half = cells // 2
    strip = 9 * depth
    f32, i32 = jnp.float32, jnp.int32
    anywhere = pl.BlockSpec(memory_space=pl.ANY)
    scalar = pl.BlockSpec(memory_space=pltpu.SMEM)
    return pl.pallas_call(
        kernel,
        out_shape=jax.ShapeDtypeStruct(populations.shape, f32),
        in_specs=[anywhere, anywhere, anywhere, scalar, scalar],
        out_specs=anywhere,
        scratch_shapes=[
            pltpu.VMEM((27, depth, rows, cells), f32),
            pltpu.VMEM((STEPS, 27, depth, rows, cells), f32),
            pltpu.VMEM((27, depth, rows, cells), f32),
            pltpu.VMEM((27, depth, rows, cells), f32),
            pltpu.VMEM((3, depth, rows, cells), f32),
            pltpu.VMEM((54, rows, half), f32),
            pltpu.VMEM((depth, rows, cells), i32),
            pltpu.VMEM((depth, rows, cells), i32),
            pltpu.VMEM((2, rows, cells), i32),
            pltpu.VMEM((2, rows, cells), i32),
            pltpu.VMEM((4, depth + 2, rows, cells), f32),
            pltpu.VMEM((2, 4, rows, cells), f32),
            pltpu.VMEM((STEPS, 2, 9, rows, cells), f32),
            pltpu.VMEM((STEPS, 2, strip, 1, cells), f32),
            pltpu.VMEM((STEPS, 2, strip, 1, cells), f32),
            pltpu.VMEM((STEPS, 4, 3, 1, cells), f32),
            pltpu.VMEM((STEPS, 4, 3, 1, cells), f32),
            pltpu.VMEM((2, 2, rows, cells), i32),
            pltpu.VMEM((2, 2, rows, cells), i32),
            pltpu.VMEM((2, 2 * depth, 1, cells), i32),
            pltpu.VMEM((2, 2 * depth, 1, cells), i32),
            pltpu.VMEM((4, 2, 1, cells), i32),
            pltpu.VMEM((4, 2, 1, cells), i32),
            pltpu.SemaphoreType.DMA((depth + 2,)),
            pltpu.SemaphoreType.DMA((depth,)),
            pltpu.SemaphoreType.DMA((STEPS + 1, ROW)),
            pltpu.SemaphoreType.DMA((STEPS + 1, ROW)),
        ],
        compiler_params=pltpu.CompilerParams(collective_id=0, has_side_effects=True),
        name="lattice_steps",
    )(populations, cell_kind, profile, vent_table.T, rates)


def solution(mesh):
    return jax.shard_map(
        local,
        mesh=mesh,
        in_specs=(
            P("scen", "gx", None, None, None),
            P("gx", None, None, "scen"),
            P("gx", None, None, "scen"),
            P("scen", None),
            P(),
        ),
        out_specs=P("scen", "gx", None, None, None),
        check_vma=False,
    )
```

```python
import jax
import jax.numpy as jnp
from jax import lax
from jax.experimental import pallas as pl
from jax.experimental.pallas import tpu as pltpu
from jax.sharding import PartitionSpec as P

PY = 8
STEPS = 3
BIG = 1e30
MESH = pl.DeviceIdType.MESH

ACROSS, CORNER, ALONG, ROW = 0, 2, 6, 12


def direction(a, b, e):
    return 9 * (a + 1) + 3 * (b + 1) + (e + 1)


def digits(k):
    return (k // 9, k // 3 % 3, k % 3)


def forward(values):
    values = list(values)
    for stride in (1, 3, 9):
        for k in range(27):
            if k // stride % 3 == 0:
                low, mid, high = (values[k], values[k + stride], values[k + 2 * stride])
                both = low + high
                values[k] = both + 4.0 * mid
                values[k + stride] = high - low
                values[k + 2 * stride] = both
    return values


def backward(values):
    values = list(values)
    for stride in (9, 3, 1):
        for k in range(27):
            if k // stride % 3 == 0:
                zero, one, two = (values[k], values[k + stride], values[k + 2 * stride])
                values[k] = two - one
                values[k + stride] = zero - 0.5 * two
                values[k + 2 * stride] = two + one
    return values


def equilibrium_moments(density, velocity):
    share = [density]
    for _ in range(3):
        share.append(share[-1] * (1.0 / 3.0))
    triple = [3.0 * component * component for component in velocity]
    result = []
    for k in range(27):
        powers = digits(k)
        ones = [axis for axis in range(3) if powers[axis] == 1]
        twos = [axis for axis in range(3) if powers[axis] == 2]
        scale = share[len(twos)]
        if len(ones) == 0:
            shape = None
            for axis in twos:
                shape = 1.0 + triple[axis] if shape is None else shape + triple[axis]
            result.append(scale if shape is None else scale * shape)
        elif len(ones) == 3:
            result.append(None)
        else:
            shape = velocity[ones[0]]
            for axis in ones[1:]:
                shape = shape * velocity[axis]
            result.append(scale * shape)
    return result


def equilibrium(velocity):
    square = velocity[0] * velocity[0] + velocity[1] * velocity[1] + velocity[2] * velocity[2]
    base = 1.0 - 1.5 * square
    result = [None] * 27
    result[13] = base
    for k in range(13):
        projected = None
        for axis, digit in enumerate(digits(k)):
            if digit != 1:
                term = velocity[axis] if digit == 2 else -velocity[axis]
                projected = term if projected is None else projected + term
        even = base + 4.5 * projected * projected
        odd = 3.0 * projected
        result[k] = even + odd
        result[26 - k] = even - odd
    return result


def shifted(main, row, b, e, lane_count):
    if b != 0:
        count = main.shape[0]
        place = lax.broadcasted_iota(jnp.int32, main.shape, 0)
        moved = pltpu.roll(main, 1 if b == 1 else count - 1, 0)
        main = jnp.where(place == (0 if b == 1 else count - 1), row, moved)
    if e != 0:
        main = pltpu.roll(main, 1 if e == 1 else lane_count - 1, 1)
    return main


def kernel(
    populations, cell_kind, profile, vent_table, rates, out,
    start, collided, passed, walls, inlet, coef, kinds, profiles,
    rim_kinds, rim_profiles, fields, rim_fields,
    get_x, put_y, get_y, put_d, get_d,
    put_kx, get_kx, put_ky, get_ky, put_kd, get_kd,
    load_sem, send_sem, recv_sem,
):
    me = lax.axis_index("gx")
    count = lax.axis_size("gx")
    depth, rows, cells = collided.shape[2], collided.shape[3], collided.shape[4]
    last = depth - 1
    half = cells // 2
    row_place = lax.rem(me + PY // 2, PY)
    right_first = lax.rem((me + PY // 2) // PY, 2) == 1
    has_row = (row_place != PY - 1, row_place != 0)

    def device(side, turn):
        place = me + count
        if side is not None:
            place = place + (PY - 2 * PY * side)
        if turn is not None:
            place = place + (1 - 2 * turn)
        return lax.rem(place, count)

    barrier = pltpu.get_barrier_semaphore()
    for side in (None, 0, 1):
        for turn in (None, 0, 1):
            if side is not None or turn is not None:
                pl.semaphore_signal(
                    barrier, inc=1, device_id={"gx": device(side, turn)}, device_id_type=MESH
                )

    order = (0, last) + tuple(range(1, last))
    loads = {}
    for x in order:
        loads[x] = pltpu.make_async_copy(populations.at[:, 0, x], start.at[:, x], load_sem.at[x])
        loads[x].start()
    kind_load = pltpu.make_async_copy(cell_kind.at[0], kinds, load_sem.at[depth])
    profile_load = pltpu.make_async_copy(profile.at[0], profiles, load_sem.at[depth + 1])
    kind_load.start()
    profile_load.start()

    def remote(source, target_ref, slot, place, side, turn):
        return pltpu.make_async_remote_copy(
            src_ref=source,
            dst_ref=target_ref,
            send_sem=send_sem.at[slot, place],
            recv_sem=recv_sem.at[slot, place],
            device_id={"gx": device(side, turn)},
            device_id_type=MESH,
        )

    def across(step, side):
        source = collided.at[step, pl.ds(18 - 18 * side, 9), last - last * side]
        return remote(source, get_x.at[step, side], step, ACROSS + side, side, None)

    def corner(step, side, turn):
        place = 2 * side + turn
        return remote(
            put_d.at[step, place], get_d.at[step, place], step, CORNER + place, side, turn
        )

    def along(step, turn, first, size, place):
        part = pl.ds(first, size)
        return remote(
            put_y.at[step, turn, part], get_y.at[step, turn, part], step,
            ALONG + 3 * turn + place, None, turn,
        )

    def along_edge(step, turn, side):
        return along(step, turn, 9 * last - (9 * last - 3) * side, 6, 2 - 2 * side)

    def along_middle(step, turn):
        return along(step, turn, 9, 9 * (last - 1), 1)

    def kind_across(side):
        return remote(put_kx.at[side], get_kx.at[side], STEPS, ACROSS + side, side, None)

    def kind_corner(side, turn):
        place = 2 * side + turn
        return remote(
            put_kd.at[place], get_kd.at[place], STEPS, CORNER + place, side, turn
        )

    def kind_along(turn):
        return remote(put_ky.at[turn], get_ky.at[turn], STEPS, ALONG + turn, None, turn)

    def go(copy, turn):
        @pl.when(has_row[turn])
        def _():
            copy().start()

    def sent(copy, turn):
        @pl.when(has_row[turn])
        def _():
            copy().wait_send()

    def came(copy, turn):
        @pl.when(has_row[1 - turn])
        def _():
            copy().wait_recv()

    for k in range(27):
        scale = 1.0
        for digit in digits(k):
            scale = scale * (0.25 if digit == 0 else 0.5)
        rate = rates[k]
        coef[2 * k] = jnp.full((rows, half), scale * (1.0 - rate), jnp.float32)
        coef[2 * k + 1] = jnp.full((rows, half), scale * rate, jnp.float32)

    def relaxed(moments, target):
        result = []
        for k in range(27):
            value = coef[2 * k] * moments[k]
            if target[k] is not None:
                value = value + coef[2 * k + 1] * target[k]
            result.append(value)
        return backward(result)

    def collide_first(x, lanes):
        moments = forward([start[k, x, :, lanes] for k in range(27)])
        density = moments[0]
        velocity = [moments[k] / density for k in (9, 3, 1)]
        result = relaxed(moments, equilibrium_moments(density, velocity))
        for k in range(27):
            collided[0, k, x, :, lanes] = result[k]

    def cell_state(step, x, lanes):
        values = [
            collided[step, k, x, :, lanes] if k == 13 else passed[k, x, :, lanes]
            for k in range(27)
        ]
        moments = forward(values)
        velocity = [moments[k] / moments[0] for k in (9, 3, 1)]
        return (values, moments, velocity, kinds[x, :, lanes])

    def collide_next(step, x, lanes):
        values, moments, velocity, kind = cell_state(step, x, lanes)
        fluid = kind == 0
        moving = fluid | (kind == 4)
        velocity = [
            jnp.where(moving, velocity[axis], inlet[axis, x, :, lanes]) for axis in range(3)
        ]
        density = jnp.where(fluid, moments[0], 216.0)
        target = equilibrium_moments(density, velocity)
        moments = [
            jnp.where(fluid, moments[k], 0.0 if target[k] is None else target[k])
            for k in range(27)
        ]
        result = relaxed(moments, target)
        for k in range(27):
            collided[step + 1, k, x, :, lanes] = result[k]

    def finish(step, x, lanes):
        values, moments, velocity, kind = cell_state(step, x, lanes)
        fluid = kind == 0
        velocity = [
            jnp.where(kind == 4, velocity[axis], inlet[axis, x, :, lanes]) for axis in range(3)
        ]
        forced = equilibrium(velocity)
        for k in range(27):
            out[k, 0, x, :, lanes] = jnp.where(fluid, values[k], forced[k])

    def by_halves(work, first, planes):
        def body(index, carry):
            plane = first + index // 2
            lanes = pl.ds(pl.multiple_of(index % 2 * half, half), half)
            work(plane, lanes)
            return carry

        lax.fori_loop(0, 2 * planes, body, 0)

    def stage_corners(step, side):
        x = last - last * side
        for turn in range(2):
            y = rows - 1 if turn == 0 else 0
            for e in range(3):
                k = 18 - 18 * side + (6 - 6 * turn) + e
                put_d[step, 2 * side + turn, e] = collided[step, k, x, pl.ds(y, 1), :]

    def stage_rows(step, x, pairs):
        for turn in range(2):
            y = rows - 1 if turn == 0 else 0
            for pair in pairs:
                k = 9 * (pair // 3) + (6 - 6 * turn) + pair % 3
                put_y[step, turn, 9 * x + pair] = collided[step, k, x, pl.ds(y, 1), :]

    def stage_edge(step, side):
        x = last - last * side
        for turn in range(2):
            y = rows - 1 if turn == 0 else 0
            for pair in range(6):
                k = 9 * (pair // 3) + 9 * side + (6 - 6 * turn) + pair % 3
                row = 9 * last - (9 * last - 3) * side + pair
                put_y[step, turn, row] = collided[step, k, x, pl.ds(y, 1), :]

    def passed_on(step, k, x, opposite, main, row, b, e):
        source = shifted(main, row, b, e, cells)
        wall = walls[k, x]
        passed[k, x] = jnp.where(wall > 0.5 * BIG, source, collided[step, opposite, x] + wall)

    def passed_middle(step, x):
        for k in range(27):
            if k == 13:
                continue
            a, b, e = (digit - 1 for digit in digits(k))
            row = None
            if b != 0:
                row = get_y[step, (1 - b) // 2, 9 * (x - a) + 3 * (a + 1) + (e + 1)]
            passed_on(step, k, x, 26 - k, collided[step, k, x - a], row, b, e)

    def passed_edge(step, side):
        x = last * side
        into, back = (18 - 18 * side, 18 * side)
        inner = x + 1 - 2 * side
        for b in (-1, 0, 1):
            turn = (1 - b) // 2
            for e in (-1, 0, 1):
                place = 3 * (b + 1) + (e + 1)
                row = None
                if b != 0:
                    row = get_d[step, 2 * side + turn, e + 1]
                passed_on(
                    step, into + place, x, back + (8 - place), get_x[step, side, place], row, b, e
                )
                if b != 0 or e != 0:
                    if b != 0:
                        row = get_y[step, turn, 9 * x + 3 + (e + 1)]
                    passed_on(
                        step, 9 + place, x, 17 - place, collided[step, 9 + place, x], row, b, e
                    )
                if b != 0:
                    row = get_y[step, turn, 9 * inner + 6 * side + (e + 1)]
                passed_on(
                    step, back + place, x, into + (8 - place),
                    collided[step, back + place, inner], row, b, e,
                )

    def field_values(kind, index):
        velocity = [jnp.zeros(kind.shape, jnp.float32) for _ in range(3)]
        for entry in range(vent_table.shape[1]):
            chosen = index == entry
            for axis in range(3):
                velocity[axis] = jnp.where(chosen, vent_table[axis, entry], velocity[axis])
        is_open = (kind == 0) | (kind >= 3)
        vent = kind == 2
        result = [jnp.where(is_open, BIG, 0.0)]
        for axis in range(3):
            result.append(jnp.where(vent, velocity[axis], 0.0))
        return result, velocity

    def prepare_walls():
        for plane in range(depth + 2):
            if plane == 0:
                kind, index = get_kx[0, 0], get_kx[0, 1]
            elif plane == depth + 1:
                kind, index = get_kx[1, 0], get_kx[1, 1]
            else:
                kind, index = kinds[plane - 1], profiles[plane - 1]
            values, velocity = field_values(kind, index)
            for field in range(4):
                fields[field, plane] = values[field]
            if 1 <= plane <= depth:
                for axis in range(3):
                    inlet[axis, plane - 1] = jnp.where(kind == 3, velocity[axis], 0.0)
        for side in range(2):
            for target, shift in ((rim_kinds, 0), (rim_profiles, 1)):
                target[side] = jnp.zeros((rows, cells), jnp.int32)
                for x in range(depth):
                    target[side, pl.ds(x + 1, 1), :] = get_ky[side, shift * depth + x]
                for row, place in ((0, side), (depth + 1, 2 + side)):
                    target[side, pl.ds(row, 1), :] = get_kd[place, shift]
            outside = row_place == (0 if side == 0 else PY - 1)
            kind = jnp.where(outside, 1, rim_kinds[side])
            values, _ = field_values(kind, rim_profiles[side])
            for field in range(4):
                rim_fields[side, field] = values[field]
        lane = lax.broadcasted_iota(jnp.int32, (rows, cells), 1)
        for plane in range(depth + 2):
            for b in (-1, 0, 1):
                for e in (-1, 0, 1):
                    moved = []
                    for field in range(4):
                        row = None
                        if b != 0:
                            row = rim_fields[0 if b == 1 else 1, field, pl.ds(plane, 1), :]
                        value = shifted(fields[field, plane], row, b, e, cells)
                        if e != 0:
                            value = jnp.where(lane == (0 if e == 1 else cells - 1), 0.0, value)
                        moved.append(value)
                    cross = moved[0]
                    if b != 0:
                        cross = cross + (6.0 * b) * moved[2]
                    if e != 0:
                        cross = cross + (6.0 * e) * moved[3]
                    for a in (-1, 0, 1):
                        x = plane - 1 + a
                        k = direction(a, b, e)
                        if 0 <= x <= last and k != 13:
                            walls[k, x] = cross if a == 0 else cross + (6.0 * a) * moved[1]

    for x in order:
        loads[x].wait()
        by_halves(collide_first, x, 1)
    for side in range(2):
        stage_corners(0, side)
        stage_edge(0, side)
    for x in range(1, last):
        stage_rows(0, x, range(9))
    kind_load.wait()
    profile_load.wait()
    for side, x in ((0, last), (1, 0)):
        put_kx[side, 0] = kinds[x]
        put_kx[side, 1] = profiles[x]
        for turn in range(2):
            y = rows - 1 if turn == 0 else 0
            put_kd[2 * side + turn, 0] = kinds[x, pl.ds(y, 1), :]
            put_kd[2 * side + turn, 1] = profiles[x, pl.ds(y, 1), :]
    for turn in range(2):
        y = rows - 1 if turn == 0 else 0
        for x in range(depth):
            put_ky[turn, x] = kinds[x, pl.ds(y, 1), :]
            put_ky[turn, depth + x] = profiles[x, pl.ds(y, 1), :]

    early = jnp.where(right_first, 0, 1)
    sides = (early, 1 - early)
    pl.semaphore_wait(barrier, 8)
    for side in sides:
        kind_across(side).start()
        for turn in range(2):
            go(lambda: kind_corner(side, turn), turn)
    for turn in range(2):
        go(lambda: kind_along(turn), turn)
    for number, side in enumerate(sides):
        if number == 1:
            across(0, sides[0]).wait_send()
        for turn in range(2):
            go(lambda: corner(0, side, turn), turn)
        across(0, side).start()
        if number == 0:
            for turn in range(2):
                go(lambda: along_middle(0, turn), turn)
                go(lambda: along_edge(0, turn, sides[0]), turn)
                go(lambda: along_edge(0, turn, sides[1]), turn)

    for side in sides:
        kind_across(side).wait_recv()
        for turn in range(2):
            came(lambda: kind_corner(side, turn), turn)
    for turn in range(2):
        came(lambda: kind_along(turn), turn)
    prepare_walls()

    for step in range(STEPS):
        final = step == STEPS - 1
        work = finish if final else collide_next

        def edge(number):
            side = sides[number]
            across(step, 1 - side).wait_recv()
            for turn in range(2):
                came(lambda: corner(step, 1 - side, turn), turn)
            passed_edge(step, 1 - side)
            x = last - last * side
            by_halves(lambda x, lanes: work(step, x, lanes), x, 1)
            if not final:
                stage_corners(step + 1, side)
                for turn in range(2):
                    go(lambda: corner(step + 1, side, turn), turn)
                stage_edge(step + 1, side)
                for turn in range(2):
                    go(lambda: along_edge(step + 1, turn, side), turn)
                across(step + 1, side).start()

        for turn in range(2):
            came(lambda: along_middle(step, turn), turn)
            came(lambda: along_edge(step, turn, sides[0]), turn)
        edge(0)
        for turn in range(2):
            came(lambda: along_edge(step, turn, sides[1]), turn)
        for x in range(1, last):
            passed_middle(step, x)
        by_halves(lambda x, lanes: work(step, x, lanes), 1, last - 1)
        if not final:
            for x in range(1, last):
                stage_rows(step + 1, x, range(9))
            for turn in range(2):
                go(lambda: along_middle(step + 1, turn), turn)
        edge(1)

    for step in range(STEPS):
        for number, side in enumerate(sides):
            if step > 0 or number == 1:
                across(step, side).wait_send()
            for turn in range(2):
                sent(lambda: corner(step, side, turn), turn)
                sent(lambda: along_edge(step, turn, side), turn)
        for turn in range(2):
            sent(lambda: along_middle(step, turn), turn)
    for side in range(2):
        kind_across(side).wait_send()
        for turn in range(2):
            sent(lambda: kind_corner(side, turn), turn)
    for turn in range(2):
        sent(lambda: kind_along(turn), turn)


def local(populations, cell_kind, profile, vent_table, rates):
    _, _, depth, rows, cells = populations.shape
    half = cells // 2
    strip = 9 * depth
    f32, i32 = jnp.float32, jnp.int32
    anywhere = pl.BlockSpec(memory_space=pl.ANY)
    scalar = pl.BlockSpec(memory_space=pltpu.SMEM)
    return pl.pallas_call(
        kernel,
        out_shape=pltpu.VMEM(populations.shape, f32),
        in_specs=[anywhere, anywhere, anywhere, scalar, scalar],
        out_specs=pl.BlockSpec(memory_space=pltpu.VMEM),
        scratch_shapes=[
            pltpu.VMEM((27, depth, rows, cells), f32),
            pltpu.VMEM((STEPS, 27, depth, rows, cells), f32),
            pltpu.VMEM((27, depth, rows, cells), f32),
            pltpu.VMEM((27, depth, rows, cells), f32),
            pltpu.VMEM((3, depth, rows, cells), f32),
            pltpu.VMEM((54, rows, half), f32),
            pltpu.VMEM((depth, rows, cells), i32),
            pltpu.VMEM((depth, rows, cells), i32),
            pltpu.VMEM((2, rows, cells), i32),
            pltpu.VMEM((2, rows, cells), i32),
            pltpu.VMEM((4, depth + 2, rows, cells), f32),
            pltpu.VMEM((2, 4, rows, cells), f32),
            pltpu.VMEM((STEPS, 2, 9, rows, cells), f32),
            pltpu.VMEM((STEPS, 2, strip, 1, cells), f32),
            pltpu.VMEM((STEPS, 2, strip, 1, cells), f32),
            pltpu.VMEM((STEPS, 4, 3, 1, cells), f32),
            pltpu.VMEM((STEPS, 4, 3, 1, cells), f32),
            pltpu.VMEM((2, 2, rows, cells), i32),
            pltpu.VMEM((2, 2, rows, cells), i32),
            pltpu.VMEM((2, 2 * depth, 1, cells), i32),
            pltpu.VMEM((2, 2 * depth, 1, cells), i32),
            pltpu.VMEM((4, 2, 1, cells), i32),
            pltpu.VMEM((4, 2, 1, cells), i32),
            pltpu.SemaphoreType.DMA((depth + 2,)),
            pltpu.SemaphoreType.DMA((STEPS + 1, ROW)),
            pltpu.SemaphoreType.DMA((STEPS + 1, ROW)),
        ],
        compiler_params=pltpu.CompilerParams(collective_id=0, has_side_effects=True),
        name="lattice_steps",
    )(populations, cell_kind, profile, vent_table.T, rates)


def solution(mesh):
    return jax.shard_map(
        local,
        mesh=mesh,
        in_specs=(
            P("scen", "gx", None, None, None),
            P("gx", None, None, "scen"),
            P("gx", None, None, "scen"),
            P("scen", None),
            P(),
        ),
        out_specs=P("scen", "gx", None, None, None),
        check_vma=False,
    )
```

```python
import jax
import jax.numpy as jnp
from jax import lax
from jax.experimental import pallas as pl
from jax.experimental.pallas import tpu as pltpu
from jax.sharding import PartitionSpec as P

PY = 8
STEPS = 3
BIG = 1e30
MESH = pl.DeviceIdType.MESH

ACROSS, CORNER, ALONG, ROW = 0, 2, 6, 12


def direction(a, b, e):
    return 9 * (a + 1) + 3 * (b + 1) + (e + 1)


def digits(k):
    return (k // 9, k // 3 % 3, k % 3)


def forward(values):
    values = list(values)
    for stride in (1, 3, 9):
        for k in range(27):
            if k // stride % 3 == 0:
                low, mid, high = (values[k], values[k + stride], values[k + 2 * stride])
                both = low + high
                values[k] = both + 4.0 * mid
                values[k + stride] = high - low
                values[k + 2 * stride] = both
    return values


def backward(values):
    values = list(values)
    for stride in (9, 3, 1):
        for k in range(27):
            if k // stride % 3 == 0:
                zero, one, two = (values[k], values[k + stride], values[k + 2 * stride])
                values[k] = two - one
                values[k + stride] = zero - 0.5 * two
                values[k + 2 * stride] = two + one
    return values


def equilibrium_moments(density, velocity):
    share = [density]
    for _ in range(3):
        share.append(share[-1] * (1.0 / 3.0))
    triple = [3.0 * component * component for component in velocity]
    result = []
    for k in range(27):
        powers = digits(k)
        ones = [axis for axis in range(3) if powers[axis] == 1]
        twos = [axis for axis in range(3) if powers[axis] == 2]
        scale = share[len(twos)]
        if len(ones) == 0:
            shape = None
            for axis in twos:
                shape = 1.0 + triple[axis] if shape is None else shape + triple[axis]
            result.append(scale if shape is None else scale * shape)
        elif len(ones) == 3:
            result.append(None)
        else:
            shape = velocity[ones[0]]
            for axis in ones[1:]:
                shape = shape * velocity[axis]
            result.append(scale * shape)
    return result


def equilibrium(velocity):
    square = velocity[0] * velocity[0] + velocity[1] * velocity[1] + velocity[2] * velocity[2]
    base = 1.0 - 1.5 * square
    result = [None] * 27
    result[13] = base
    for k in range(13):
        projected = None
        for axis, digit in enumerate(digits(k)):
            if digit != 1:
                term = velocity[axis] if digit == 2 else -velocity[axis]
                projected = term if projected is None else projected + term
        even = base + 4.5 * projected * projected
        odd = 3.0 * projected
        result[k] = even + odd
        result[26 - k] = even - odd
    return result


def shifted(main, row, b, e, lane_count):
    if b != 0:
        count = main.shape[0]
        place = lax.broadcasted_iota(jnp.int32, main.shape, 0)
        moved = pltpu.roll(main, 1 if b == 1 else count - 1, 0)
        main = jnp.where(place == (0 if b == 1 else count - 1), row, moved)
    if e != 0:
        main = pltpu.roll(main, 1 if e == 1 else lane_count - 1, 1)
    return main


def kernel(
    populations, cell_kind, profile, vent_table, rates, out,
    start, collided, passed, walls, inlet, coef, kinds, profiles,
    rim_kinds, rim_profiles, fields, rim_fields,
    get_x, put_y, get_y, put_d, get_d,
    put_kx, get_kx, put_ky, get_ky, put_kd, get_kd,
    load_sem, send_sem, recv_sem,
):
    me = lax.axis_index("gx")
    count = lax.axis_size("gx")
    depth, rows, cells = collided.shape[2], collided.shape[3], collided.shape[4]
    last = depth - 1
    half = cells // 2
    row_place = lax.rem(me + PY // 2, PY)
    right_first = lax.rem((me + PY // 2) // PY, 2) == 1
    has_row = (row_place != PY - 1, row_place != 0)

    def device(side, turn):
        place = me + count
        if side is not None:
            place = place + (PY - 2 * PY * side)
        if turn is not None:
            place = place + (1 - 2 * turn)
        return lax.rem(place, count)

    barrier = pltpu.get_barrier_semaphore()
    for side in (None, 0, 1):
        for turn in (None, 0, 1):
            if side is not None or turn is not None:
                pl.semaphore_signal(
                    barrier, inc=1, device_id={"gx": device(side, turn)}, device_id_type=MESH
                )

    order = (0, last) + tuple(range(1, last))
    loads = {}
    for x in order:
        loads[x] = pltpu.make_async_copy(populations.at[:, 0, x], start.at[:, x], load_sem.at[x])
        loads[x].start()
    kind_load = pltpu.make_async_copy(cell_kind.at[0], kinds, load_sem.at[depth])
    profile_load = pltpu.make_async_copy(profile.at[0], profiles, load_sem.at[depth + 1])
    kind_load.start()
    profile_load.start()

    def remote(source, target_ref, slot, place, side, turn):
        return pltpu.make_async_remote_copy(
            src_ref=source,
            dst_ref=target_ref,
            send_sem=send_sem.at[slot, place],
            recv_sem=recv_sem.at[slot, place],
            device_id={"gx": device(side, turn)},
            device_id_type=MESH,
        )

    def across(step, side):
        source = collided.at[step, pl.ds(18 - 18 * side, 9), last - last * side]
        return remote(source, get_x.at[step, side], step, ACROSS + side, side, None)

    def across_go(step, side):
        for first in range(0, 9, 1):
            source = collided.at[step, pl.ds(18 - 18 * side + first, 1), last - last * side]
            target = get_x.at[step, side, pl.ds(first, 1)]
            remote(source, target, step, ACROSS + side, side, None).start()

    def corner(step, side, turn):
        place = 2 * side + turn
        return remote(
            put_d.at[step, place], get_d.at[step, place], step, CORNER + place, side, turn
        )

    def along(step, turn, first, size, place):
        part = pl.ds(first, size)
        return remote(
            put_y.at[step, turn, part], get_y.at[step, turn, part], step,
            ALONG + 3 * turn + place, None, turn,
        )

    def along_edge(step, turn, side):
        return along(step, turn, 9 * last - (9 * last - 3) * side, 6, 2 - 2 * side)

    def along_middle(step, turn):
        return along(step, turn, 9, 9 * (last - 1), 1)

    def kind_across(side):
        return remote(put_kx.at[side], get_kx.at[side], STEPS, ACROSS + side, side, None)

    def kind_corner(side, turn):
        place = 2 * side + turn
        return remote(
            put_kd.at[place], get_kd.at[place], STEPS, CORNER + place, side, turn
        )

    def kind_along(turn):
        return remote(put_ky.at[turn], get_ky.at[turn], STEPS, ALONG + turn, None, turn)

    def go(copy, turn):
        @pl.when(has_row[turn])
        def _():
            copy().start()

    def sent(copy, turn):
        @pl.when(has_row[turn])
        def _():
            copy().wait_send()

    def came(copy, turn):
        @pl.when(has_row[1 - turn])
        def _():
            copy().wait_recv()

    for k in range(27):
        scale = 1.0
        for digit in digits(k):
            scale = scale * (0.25 if digit == 0 else 0.5)
        rate = rates[k]
        coef[2 * k] = jnp.full((rows, half), scale * (1.0 - rate), jnp.float32)
        coef[2 * k + 1] = jnp.full((rows, half), scale * rate, jnp.float32)

    def relaxed(moments, target):
        result = []
        for k in range(27):
            value = coef[2 * k] * moments[k]
            if target[k] is not None:
                value = value + coef[2 * k + 1] * target[k]
            result.append(value)
        return backward(result)

    def collide_first(x, lanes):
        moments = forward([start[k, x, :, lanes] for k in range(27)])
        density = moments[0]
        velocity = [moments[k] / density for k in (9, 3, 1)]
        result = relaxed(moments, equilibrium_moments(density, velocity))
        for k in range(27):
            collided[0, k, x, :, lanes] = result[k]

    def cell_state(step, x, lanes):
        values = [
            collided[step, k, x, :, lanes] if k == 13 else passed[k, x, :, lanes]
            for k in range(27)
        ]
        moments = forward(values)
        velocity = [moments[k] / moments[0] for k in (9, 3, 1)]
        return (values, moments, velocity, kinds[x, :, lanes])

    def collide_next(step, x, lanes):
        values, moments, velocity, kind = cell_state(step, x, lanes)
        fluid = kind == 0
        moving = fluid | (kind == 4)
        velocity = [
            jnp.where(moving, velocity[axis], inlet[axis, x, :, lanes]) for axis in range(3)
        ]
        density = jnp.where(fluid, moments[0], 216.0)
        target = equilibrium_moments(density, velocity)
        moments = [
            jnp.where(fluid, moments[k], 0.0 if target[k] is None else target[k])
            for k in range(27)
        ]
        result = relaxed(moments, target)
        for k in range(27):
            collided[step + 1, k, x, :, lanes] = result[k]

    def finish(step, x, lanes):
        values, moments, velocity, kind = cell_state(step, x, lanes)
        fluid = kind == 0
        velocity = [
            jnp.where(kind == 4, velocity[axis], inlet[axis, x, :, lanes]) for axis in range(3)
        ]
        forced = equilibrium(velocity)
        for k in range(27):
            out[k, 0, x, :, lanes] = jnp.where(fluid, values[k], forced[k])

    def by_halves(work, first, planes):
        def body(index, carry):
            plane = first + index // 2
            lanes = pl.ds(pl.multiple_of(index % 2 * half, half), half)
            work(plane, lanes)
            return carry

        lax.fori_loop(0, 2 * planes, body, 0)

    def stage_corners(step, side):
        x = last - last * side
        for turn in range(2):
            y = rows - 1 if turn == 0 else 0
            for e in range(3):
                k = 18 - 18 * side + (6 - 6 * turn) + e
                put_d[step, 2 * side + turn, e] = collided[step, k, x, pl.ds(y, 1), :]

    def stage_rows(step, x, pairs):
        for turn in range(2):
            y = rows - 1 if turn == 0 else 0
            for pair in pairs:
                k = 9 * (pair // 3) + (6 - 6 * turn) + pair % 3
                put_y[step, turn, 9 * x + pair] = collided[step, k, x, pl.ds(y, 1), :]

    def stage_edge(step, side):
        x = last - last * side
        for turn in range(2):
            y = rows - 1 if turn == 0 else 0
            for pair in range(6):
                k = 9 * (pair // 3) + 9 * side + (6 - 6 * turn) + pair % 3
                row = 9 * last - (9 * last - 3) * side + pair
                put_y[step, turn, row] = collided[step, k, x, pl.ds(y, 1), :]

    def passed_on(step, k, x, opposite, main, row, b, e):
        source = shifted(main, row, b, e, cells)
        wall = walls[k, x]
        passed[k, x] = jnp.where(wall > 0.5 * BIG, source, collided[step, opposite, x] + wall)

    def passed_middle(step, x):
        for k in range(27):
            if k == 13:
                continue
            a, b, e = (digit - 1 for digit in digits(k))
            row = None
            if b != 0:
                row = get_y[step, (1 - b) // 2, 9 * (x - a) + 3 * (a + 1) + (e + 1)]
            passed_on(step, k, x, 26 - k, collided[step, k, x - a], row, b, e)

    def passed_edge(step, side):
        x = last * side
        into, back = (18 - 18 * side, 18 * side)
        inner = x + 1 - 2 * side
        for b in (-1, 0, 1):
            turn = (1 - b) // 2
            for e in (-1, 0, 1):
                place = 3 * (b + 1) + (e + 1)
                row = None
                if b != 0:
                    row = get_d[step, 2 * side + turn, e + 1]
                passed_on(
                    step, into + place, x, back + (8 - place), get_x[step, side, place], row, b, e
                )
                if b != 0 or e != 0:
                    if b != 0:
                        row = get_y[step, turn, 9 * x + 3 + (e + 1)]
                    passed_on(
                        step, 9 + place, x, 17 - place, collided[step, 9 + place, x], row, b, e
                    )
                if b != 0:
                    row = get_y[step, turn, 9 * inner + 6 * side + (e + 1)]
                passed_on(
                    step, back + place, x, into + (8 - place),
                    collided[step, back + place, inner], row, b, e,
                )

    def field_values(kind, index):
        velocity = [jnp.zeros(kind.shape, jnp.float32) for _ in range(3)]
        for entry in range(vent_table.shape[1]):
            chosen = index == entry
            for axis in range(3):
                velocity[axis] = jnp.where(chosen, vent_table[axis, entry], velocity[axis])
        is_open = (kind == 0) | (kind >= 3)
        vent = kind == 2
        result = [jnp.where(is_open, BIG, 0.0)]
        for axis in range(3):
            result.append(jnp.where(vent, velocity[axis], 0.0))
        return result, velocity

    def prepare_walls():
        for plane in range(depth + 2):
            if plane == 0:
                kind, index = get_kx[0, 0], get_kx[0, 1]
            elif plane == depth + 1:
                kind, index = get_kx[1, 0], get_kx[1, 1]
            else:
                kind, index = kinds[plane - 1], profiles[plane - 1]
            values, velocity = field_values(kind, index)
            for field in range(4):
                fields[field, plane] = values[field]
            if 1 <= plane <= depth:
                for axis in range(3):
                    inlet[axis, plane - 1] = jnp.where(kind == 3, velocity[axis], 0.0)
        for side in range(2):
            for target, shift in ((rim_kinds, 0), (rim_profiles, 1)):
                target[side] = jnp.zeros((rows, cells), jnp.int32)
                for x in range(depth):
                    target[side, pl.ds(x + 1, 1), :] = get_ky[side, shift * depth + x]
                for row, place in ((0, side), (depth + 1, 2 + side)):
                    target[side, pl.ds(row, 1), :] = get_kd[place, shift]
            outside = row_place == (0 if side == 0 else PY - 1)
            kind = jnp.where(outside, 1, rim_kinds[side])
            values, _ = field_values(kind, rim_profiles[side])
            for field in range(4):
                rim_fields[side, field] = values[field]
        lane = lax.broadcasted_iota(jnp.int32, (rows, cells), 1)
        for plane in range(depth + 2):
            for b in (-1, 0, 1):
                for e in (-1, 0, 1):
                    moved = []
                    for field in range(4):
                        row = None
                        if b != 0:
                            row = rim_fields[0 if b == 1 else 1, field, pl.ds(plane, 1), :]
                        value = shifted(fields[field, plane], row, b, e, cells)
                        if e != 0:
                            value = jnp.where(lane == (0 if e == 1 else cells - 1), 0.0, value)
                        moved.append(value)
                    cross = moved[0]
                    if b != 0:
                        cross = cross + (6.0 * b) * moved[2]
                    if e != 0:
                        cross = cross + (6.0 * e) * moved[3]
                    for a in (-1, 0, 1):
                        x = plane - 1 + a
                        k = direction(a, b, e)
                        if 0 <= x <= last and k != 13:
                            walls[k, x] = cross if a == 0 else cross + (6.0 * a) * moved[1]

    for x in order:
        loads[x].wait()
        by_halves(collide_first, x, 1)
    for side in range(2):
        stage_corners(0, side)
        stage_edge(0, side)
    for x in range(1, last):
        stage_rows(0, x, range(9))
    kind_load.wait()
    profile_load.wait()
    for side, x in ((0, last), (1, 0)):
        put_kx[side, 0] = kinds[x]
        put_kx[side, 1] = profiles[x]
        for turn in range(2):
            y = rows - 1 if turn == 0 else 0
            put_kd[2 * side + turn, 0] = kinds[x, pl.ds(y, 1), :]
            put_kd[2 * side + turn, 1] = profiles[x, pl.ds(y, 1), :]
    for turn in range(2):
        y = rows - 1 if turn == 0 else 0
        for x in range(depth):
            put_ky[turn, x] = kinds[x, pl.ds(y, 1), :]
            put_ky[turn, depth + x] = profiles[x, pl.ds(y, 1), :]

    early = jnp.where(right_first, 0, 1)
    sides = (early, 1 - early)
    pl.semaphore_wait(barrier, 8)
    for side in sides:
        kind_across(side).start()
        for turn in range(2):
            go(lambda: kind_corner(side, turn), turn)
    for turn in range(2):
        go(lambda: kind_along(turn), turn)
    for number, side in enumerate(sides):
        if number == 1:
            across(0, sides[0]).wait_send()
        for turn in range(2):
            go(lambda: corner(0, side, turn), turn)
        across_go(0, side)
        if number == 0:
            for turn in range(2):
                go(lambda: along_middle(0, turn), turn)
                go(lambda: along_edge(0, turn, sides[0]), turn)
                go(lambda: along_edge(0, turn, sides[1]), turn)

    for side in sides:
        kind_across(side).wait_recv()
        for turn in range(2):
            came(lambda: kind_corner(side, turn), turn)
    for turn in range(2):
        came(lambda: kind_along(turn), turn)
    prepare_walls()

    def all_sent(step):
        for number, side in enumerate(sides):
            if step > 0 or number == 1:
                across(step, side).wait_send()
            for turn in range(2):
                sent(lambda: corner(step, side, turn), turn)
                sent(lambda: along_edge(step, turn, side), turn)
        for turn in range(2):
            sent(lambda: along_middle(step, turn), turn)

    for step in range(STEPS):
        final = step == STEPS - 1
        work = finish if final else collide_next
        if final:
            for earlier in range(step):
                all_sent(earlier)
            for side in range(2):
                kind_across(side).wait_send()
                for turn in range(2):
                    sent(lambda: kind_corner(side, turn), turn)
            for turn in range(2):
                sent(lambda: kind_along(turn), turn)

        def edge(number):
            side = sides[number]
            across(step, 1 - side).wait_recv()
            for turn in range(2):
                came(lambda: corner(step, 1 - side, turn), turn)
            passed_edge(step, 1 - side)
            x = last - last * side
            by_halves(lambda x, lanes: work(step, x, lanes), x, 1)
            if not final:
                stage_corners(step + 1, side)
                for turn in range(2):
                    go(lambda: corner(step + 1, side, turn), turn)
                stage_edge(step + 1, side)
                for turn in range(2):
                    go(lambda: along_edge(step + 1, turn, side), turn)
                across_go(step + 1, side)

        for turn in range(2):
            came(lambda: along_middle(step, turn), turn)
            came(lambda: along_edge(step, turn, sides[0]), turn)
        edge(0)
        for turn in range(2):
            came(lambda: along_edge(step, turn, sides[1]), turn)
        for x in range(1, last):
            passed_middle(step, x)
        by_halves(lambda x, lanes: work(step, x, lanes), 1, last - 1)
        if not final:
            for x in range(1, last):
                stage_rows(step + 1, x, range(9))
            for turn in range(2):
                go(lambda: along_middle(step + 1, turn), turn)
        edge(1)

    all_sent(STEPS - 1)


def local(populations, cell_kind, profile, vent_table, rates):
    _, _, depth, rows, cells = populations.shape
    half = cells // 2
    strip = 9 * depth
    f32, i32 = jnp.float32, jnp.int32
    anywhere = pl.BlockSpec(memory_space=pl.ANY)
    scalar = pl.BlockSpec(memory_space=pltpu.SMEM)
    return pl.pallas_call(
        kernel,
        out_shape=pltpu.VMEM(populations.shape, f32),
        in_specs=[anywhere, anywhere, anywhere, scalar, scalar],
        out_specs=pl.BlockSpec(memory_space=pltpu.VMEM),
        scratch_shapes=[
            pltpu.VMEM((27, depth, rows, cells), f32),
            pltpu.VMEM((STEPS, 27, depth, rows, cells), f32),
            pltpu.VMEM((27, depth, rows, cells), f32),
            pltpu.VMEM((27, depth, rows, cells), f32),
            pltpu.VMEM((3, depth, rows, cells), f32),
            pltpu.VMEM((54, rows, half), f32),
            pltpu.VMEM((depth, rows, cells), i32),
            pltpu.VMEM((depth, rows, cells), i32),
            pltpu.VMEM((2, rows, cells), i32),
            pltpu.VMEM((2, rows, cells), i32),
            pltpu.VMEM((4, depth + 2, rows, cells), f32),
            pltpu.VMEM((2, 4, rows, cells), f32),
            pltpu.VMEM((STEPS, 2, 9, rows, cells), f32),
            pltpu.VMEM((STEPS, 2, strip, 1, cells), f32),
            pltpu.VMEM((STEPS, 2, strip, 1, cells), f32),
            pltpu.VMEM((STEPS, 4, 3, 1, cells), f32),
            pltpu.VMEM((STEPS, 4, 3, 1, cells), f32),
            pltpu.VMEM((2, 2, rows, cells), i32),
            pltpu.VMEM((2, 2, rows, cells), i32),
            pltpu.VMEM((2, 2 * depth, 1, cells), i32),
            pltpu.VMEM((2, 2 * depth, 1, cells), i32),
            pltpu.VMEM((4, 2, 1, cells), i32),
            pltpu.VMEM((4, 2, 1, cells), i32),
            pltpu.SemaphoreType.DMA((depth + 2,)),
            pltpu.SemaphoreType.DMA((STEPS + 1, ROW)),
            pltpu.SemaphoreType.DMA((STEPS + 1, ROW)),
        ],
        compiler_params=pltpu.CompilerParams(collective_id=0, has_side_effects=True),
        name="lattice_steps",
    )(populations, cell_kind, profile, vent_table.T, rates)


def solution(mesh):
    return jax.shard_map(
        local,
        mesh=mesh,
        in_specs=(
            P("scen", "gx", None, None, None),
            P("gx", None, None, "scen"),
            P("gx", None, None, "scen"),
            P("scen", None),
            P(),
        ),
        out_specs=P("scen", "gx", None, None, None),
        check_vma=False,
    )
```

```python
import jax
import jax.numpy as jnp
from jax import lax
from jax.experimental import pallas as pl
from jax.experimental.pallas import tpu as pltpu
from jax.sharding import PartitionSpec as P

PY = 8
STEPS = 3
BIG = 1e30
MESH = pl.DeviceIdType.MESH

ACROSS, CORNER, ALONG, ROW = 0, 2, 6, 12


def direction(a, b, e):
    return 9 * (a + 1) + 3 * (b + 1) + (e + 1)


def digits(k):
    return (k // 9, k // 3 % 3, k % 3)


def forward(values):
    values = list(values)
    for stride in (1, 3, 9):
        for k in range(27):
            if k // stride % 3 == 0:
                low, mid, high = (values[k], values[k + stride], values[k + 2 * stride])
                both = low + high
                values[k] = both + 4.0 * mid
                values[k + stride] = high - low
                values[k + 2 * stride] = both
    return values


def backward(values):
    values = list(values)
    for stride in (9, 3, 1):
        for k in range(27):
            if k // stride % 3 == 0:
                zero, one, two = (values[k], values[k + stride], values[k + 2 * stride])
                values[k] = two - one
                values[k + stride] = zero - 0.5 * two
                values[k + 2 * stride] = two + one
    return values


def equilibrium_moments(density, velocity):
    share = [density]
    for _ in range(3):
        share.append(share[-1] * (1.0 / 3.0))
    triple = [3.0 * component * component for component in velocity]
    result = []
    for k in range(27):
        powers = digits(k)
        ones = [axis for axis in range(3) if powers[axis] == 1]
        twos = [axis for axis in range(3) if powers[axis] == 2]
        scale = share[len(twos)]
        if len(ones) == 0:
            shape = None
            for axis in twos:
                shape = 1.0 + triple[axis] if shape is None else shape + triple[axis]
            result.append(scale if shape is None else scale * shape)
        elif len(ones) == 3:
            result.append(None)
        else:
            shape = velocity[ones[0]]
            for axis in ones[1:]:
                shape = shape * velocity[axis]
            result.append(scale * shape)
    return result


def equilibrium(velocity):
    square = velocity[0] * velocity[0] + velocity[1] * velocity[1] + velocity[2] * velocity[2]
    base = 1.0 - 1.5 * square
    result = [None] * 27
    result[13] = base
    for k in range(13):
        projected = None
        for axis, digit in enumerate(digits(k)):
            if digit != 1:
                term = velocity[axis] if digit == 2 else -velocity[axis]
                projected = term if projected is None else projected + term
        even = base + 4.5 * projected * projected
        odd = 3.0 * projected
        result[k] = even + odd
        result[26 - k] = even - odd
    return result


def shifted(main, row, b, e, lane_count):
    if b != 0:
        count = main.shape[0]
        place = lax.broadcasted_iota(jnp.int32, main.shape, 0)
        moved = pltpu.roll(main, 1 if b == 1 else count - 1, 0)
        main = jnp.where(place == (0 if b == 1 else count - 1), row, moved)
    if e != 0:
        main = pltpu.roll(main, 1 if e == 1 else lane_count - 1, 1)
    return main


def kernel(
    populations, cell_kind, profile, vent_table, rates, out,
    start, collided, passed, walls, inlet, coef, kinds, profiles,
    rim_kinds, rim_profiles, fields, rim_fields,
    get_x, put_y, get_y, put_d, get_d,
    put_kx, get_kx, put_ky, get_ky, put_kd, get_kd,
    load_sem, send_sem, recv_sem,
):
    me = lax.axis_index("gx")
    count = lax.axis_size("gx")
    depth, rows, cells = collided.shape[2], collided.shape[3], collided.shape[4]
    last = depth - 1
    half = cells // 2
    row_place = lax.rem(me + PY // 2, PY)
    right_first = lax.rem((me + PY // 2) // PY, 2) == 1
    has_row = (row_place != PY - 1, row_place != 0)

    def device(side, turn):
        place = me + count
        if side is not None:
            place = place + (PY - 2 * PY * side)
        if turn is not None:
            place = place + (1 - 2 * turn)
        return lax.rem(place, count)

    barrier = pltpu.get_barrier_semaphore()
    for side in (None, 0, 1):
        for turn in (None, 0, 1):
            if side is not None or turn is not None:
                pl.semaphore_signal(
                    barrier, inc=1, device_id={"gx": device(side, turn)}, device_id_type=MESH
                )

    order = (0, last) + tuple(range(1, last))
    loads = {}
    for x in order:
        loads[x] = pltpu.make_async_copy(populations.at[:, 0, x], start.at[:, x], load_sem.at[x])
        loads[x].start()
    kind_load = pltpu.make_async_copy(cell_kind.at[0], kinds, load_sem.at[depth])
    profile_load = pltpu.make_async_copy(profile.at[0], profiles, load_sem.at[depth + 1])
    kind_load.start()
    profile_load.start()

    def remote(source, target_ref, slot, place, side, turn):
        return pltpu.make_async_remote_copy(
            src_ref=source,
            dst_ref=target_ref,
            send_sem=send_sem.at[slot, place],
            recv_sem=recv_sem.at[slot, place],
            device_id={"gx": device(side, turn)},
            device_id_type=MESH,
        )

    def across(step, side):
        source = collided.at[step, pl.ds(18 - 18 * side, 9), last - last * side]
        return remote(source, get_x.at[step, side], step, ACROSS + side, side, None)

    def across_go(step, side):
        for first in range(0, 9, 1):
            source = collided.at[step, pl.ds(18 - 18 * side + first, 1), last - last * side]
            target = get_x.at[step, side, pl.ds(first, 1)]
            remote(source, target, step, ACROSS + side, side, None).start()

    def corner(step, side, turn):
        place = 2 * side + turn
        return remote(
            put_d.at[step, place], get_d.at[step, place], step, CORNER + place, side, turn
        )

    def along(step, turn, first, size, place):
        part = pl.ds(first, size)
        return remote(
            put_y.at[step, turn, part], get_y.at[step, turn, part], step,
            ALONG + 3 * turn + place, None, turn,
        )

    def along_edge(step, turn, side):
        return along(step, turn, 9 * last - (9 * last - 3) * side, 6, 2 - 2 * side)

    def along_middle(step, turn):
        return along(step, turn, 9, 9 * (last - 1), 1)

    def kind_across(side):
        return remote(put_kx.at[side], get_kx.at[side], STEPS, ACROSS + side, side, None)

    def kind_corner(side, turn):
        place = 2 * side + turn
        return remote(
            put_kd.at[place], get_kd.at[place], STEPS, CORNER + place, side, turn
        )

    def kind_along(turn):
        return remote(put_ky.at[turn], get_ky.at[turn], STEPS, ALONG + turn, None, turn)

    def go(copy, turn):
        @pl.when(has_row[turn])
        def _():
            copy().start()

    def sent(copy, turn):
        @pl.when(has_row[turn])
        def _():
            copy().wait_send()

    def came(copy, turn):
        @pl.when(has_row[1 - turn])
        def _():
            copy().wait_recv()

    for k in range(27):
        scale = 1.0
        for digit in digits(k):
            scale = scale * (0.25 if digit == 0 else 0.5)
        rate = rates[k]
        coef[2 * k] = jnp.full((rows, half), scale * (1.0 - rate), jnp.float32)
        coef[2 * k + 1] = jnp.full((rows, half), scale * rate, jnp.float32)

    def relaxed(moments, target):
        result = []
        for k in range(27):
            value = coef[2 * k] * moments[k]
            if target[k] is not None:
                value = value + coef[2 * k + 1] * target[k]
            result.append(value)
        return backward(result)

    def collide_first(x, lanes):
        moments = forward([start[k, x, :, lanes] for k in range(27)])
        density = moments[0]
        velocity = [moments[k] / density for k in (9, 3, 1)]
        result = relaxed(moments, equilibrium_moments(density, velocity))
        for k in range(27):
            collided[0, k, x, :, lanes] = result[k]

    def cell_state(step, x, lanes):
        values = [
            collided[step, k, x, :, lanes] if k == 13 else passed[k, x, :, lanes]
            for k in range(27)
        ]
        moments = forward(values)
        velocity = [moments[k] / moments[0] for k in (9, 3, 1)]
        return (values, moments, velocity, kinds[x, :, lanes])

    def collide_next(step, x, lanes):
        values, moments, velocity, kind = cell_state(step, x, lanes)
        fluid = kind == 0
        moving = fluid | (kind == 4)
        velocity = [
            jnp.where(moving, velocity[axis], inlet[axis, x, :, lanes]) for axis in range(3)
        ]
        density = jnp.where(fluid, moments[0], 216.0)
        target = equilibrium_moments(density, velocity)
        moments = [
            jnp.where(fluid, moments[k], 0.0 if target[k] is None else target[k])
            for k in range(27)
        ]
        result = relaxed(moments, target)
        for k in range(27):
            collided[step + 1, k, x, :, lanes] = result[k]

    def finish(step, x, lanes):
        values, moments, velocity, kind = cell_state(step, x, lanes)
        fluid = kind == 0
        velocity = [
            jnp.where(kind == 4, velocity[axis], inlet[axis, x, :, lanes]) for axis in range(3)
        ]
        forced = equilibrium(velocity)
        for k in range(27):
            out[k, 0, x, :, lanes] = jnp.where(fluid, values[k], forced[k])

    def by_halves(work, first, planes):
        def body(index, carry):
            plane = first + index // 2
            lanes = pl.ds(pl.multiple_of(index % 2 * half, half), half)
            work(plane, lanes)
            return carry

        lax.fori_loop(0, 2 * planes, body, 0)

    def stage_corners(step, side):
        x = last - last * side
        for turn in range(2):
            y = rows - 1 if turn == 0 else 0
            for e in range(3):
                k = 18 - 18 * side + (6 - 6 * turn) + e
                put_d[step, 2 * side + turn, e] = collided[step, k, x, pl.ds(y, 1), :]

    def stage_rows(step, x, pairs):
        for turn in range(2):
            y = rows - 1 if turn == 0 else 0
            for pair in pairs:
                k = 9 * (pair // 3) + (6 - 6 * turn) + pair % 3
                put_y[step, turn, 9 * x + pair] = collided[step, k, x, pl.ds(y, 1), :]

    def stage_edge(step, side):
        x = last - last * side
        for turn in range(2):
            y = rows - 1 if turn == 0 else 0
            for pair in range(6):
                k = 9 * (pair // 3) + 9 * side + (6 - 6 * turn) + pair % 3
                row = 9 * last - (9 * last - 3) * side + pair
                put_y[step, turn, row] = collided[step, k, x, pl.ds(y, 1), :]

    def passed_on(step, k, x, opposite, main, row, b, e):
        source = shifted(main, row, b, e, cells)
        wall = walls[k, x]
        passed[k, x] = jnp.where(wall > 0.5 * BIG, source, collided[step, opposite, x] + wall)

    def passed_middle(step, x):
        for k in range(27):
            if k == 13:
                continue
            a, b, e = (digit - 1 for digit in digits(k))
            row = None
            if b != 0:
                row = get_y[step, (1 - b) // 2, 9 * (x - a) + 3 * (a + 1) + (e + 1)]
            passed_on(step, k, x, 26 - k, collided[step, k, x - a], row, b, e)

    def passed_edge_own(step, side):
        x = last * side
        into, back = (18 - 18 * side, 18 * side)
        inner = x + 1 - 2 * side
        for b in (-1, 0, 1):
            turn = (1 - b) // 2
            for e in (-1, 0, 1):
                place = 3 * (b + 1) + (e + 1)
                row = None
                if b != 0 or e != 0:
                    if b != 0:
                        row = get_y[step, turn, 9 * x + 3 + (e + 1)]
                    passed_on(
                        step, 9 + place, x, 17 - place, collided[step, 9 + place, x], row, b, e
                    )
                if b != 0:
                    row = get_y[step, turn, 9 * inner + 6 * side + (e + 1)]
                passed_on(
                    step, back + place, x, into + (8 - place),
                    collided[step, back + place, inner], row, b, e,
                )

    def passed_edge(step, side):
        x = last * side
        into, back = (18 - 18 * side, 18 * side)
        for b in (-1, 0, 1):
            turn = (1 - b) // 2
            for e in (-1, 0, 1):
                place = 3 * (b + 1) + (e + 1)
                row = None
                if b != 0:
                    row = get_d[step, 2 * side + turn, e + 1]
                passed_on(
                    step, into + place, x, back + (8 - place), get_x[step, side, place], row, b, e
                )

    def field_values(kind, index):
        velocity = [jnp.zeros(kind.shape, jnp.float32) for _ in range(3)]
        for entry in range(vent_table.shape[1]):
            chosen = index == entry
            for axis in range(3):
                velocity[axis] = jnp.where(chosen, vent_table[axis, entry], velocity[axis])
        is_open = (kind == 0) | (kind >= 3)
        vent = kind == 2
        result = [jnp.where(is_open, BIG, 0.0)]
        for axis in range(3):
            result.append(jnp.where(vent, velocity[axis], 0.0))
        return result, velocity

    def prepare_fields():
        for x in range(depth):
            values, velocity = field_values(kinds[x], profiles[x])
            for field in range(4):
                fields[field, x + 1] = values[field]
            for axis in range(3):
                inlet[axis, x] = jnp.where(kinds[x] == 3, velocity[axis], 0.0)

    def prepare_walls():
        for plane, side in ((0, 0), (depth + 1, 1)):
            values, _ = field_values(get_kx[side, 0], get_kx[side, 1])
            for field in range(4):
                fields[field, plane] = values[field]
        for side in range(2):
            for target, shift in ((rim_kinds, 0), (rim_profiles, 1)):
                target[side] = jnp.zeros((rows, cells), jnp.int32)
                for x in range(depth):
                    target[side, pl.ds(x + 1, 1), :] = get_ky[side, shift * depth + x]
                for row, place in ((0, side), (depth + 1, 2 + side)):
                    target[side, pl.ds(row, 1), :] = get_kd[place, shift]
            outside = row_place == (0 if side == 0 else PY - 1)
            kind = jnp.where(outside, 1, rim_kinds[side])
            values, _ = field_values(kind, rim_profiles[side])
            for field in range(4):
                rim_fields[side, field] = values[field]
        lane = lax.broadcasted_iota(jnp.int32, (rows, cells), 1)
        for plane in range(depth + 2):
            for b in (-1, 0, 1):
                for e in (-1, 0, 1):
                    moved = []
                    for field in range(4):
                        row = None
                        if b != 0:
                            row = rim_fields[0 if b == 1 else 1, field, pl.ds(plane, 1), :]
                        value = shifted(fields[field, plane], row, b, e, cells)
                        if e != 0:
                            value = jnp.where(lane == (0 if e == 1 else cells - 1), 0.0, value)
                        moved.append(value)
                    cross = moved[0]
                    if b != 0:
                        cross = cross + (6.0 * b) * moved[2]
                    if e != 0:
                        cross = cross + (6.0 * e) * moved[3]
                    for a in (-1, 0, 1):
                        x = plane - 1 + a
                        k = direction(a, b, e)
                        if 0 <= x <= last and k != 13:
                            walls[k, x] = cross if a == 0 else cross + (6.0 * a) * moved[1]

    for x in order:
        loads[x].wait()
        by_halves(collide_first, x, 1)
    for side in range(2):
        stage_corners(0, side)
        stage_edge(0, side)
    for x in range(1, last):
        stage_rows(0, x, range(9))
    kind_load.wait()
    profile_load.wait()
    for side, x in ((0, last), (1, 0)):
        put_kx[side, 0] = kinds[x]
        put_kx[side, 1] = profiles[x]
        for turn in range(2):
            y = rows - 1 if turn == 0 else 0
            put_kd[2 * side + turn, 0] = kinds[x, pl.ds(y, 1), :]
            put_kd[2 * side + turn, 1] = profiles[x, pl.ds(y, 1), :]
    for turn in range(2):
        y = rows - 1 if turn == 0 else 0
        for x in range(depth):
            put_ky[turn, x] = kinds[x, pl.ds(y, 1), :]
            put_ky[turn, depth + x] = profiles[x, pl.ds(y, 1), :]

    early = jnp.where(right_first, 0, 1)
    sides = (early, 1 - early)
    pl.semaphore_wait(barrier, 8)
    for side in sides:
        kind_across(side).start()
        for turn in range(2):
            go(lambda: kind_corner(side, turn), turn)
    for turn in range(2):
        go(lambda: kind_along(turn), turn)
    for number, side in enumerate(sides):
        if number == 1:
            across(0, sides[0]).wait_send()
        for turn in range(2):
            go(lambda: corner(0, side, turn), turn)
        across_go(0, side)
        if number == 0:
            for turn in range(2):
                go(lambda: along_middle(0, turn), turn)
                go(lambda: along_edge(0, turn, sides[0]), turn)
                go(lambda: along_edge(0, turn, sides[1]), turn)

    prepare_fields()
    for side in sides:
        kind_across(side).wait_recv()
        for turn in range(2):
            came(lambda: kind_corner(side, turn), turn)
    for turn in range(2):
        came(lambda: kind_along(turn), turn)
    prepare_walls()

    def all_sent(step):
        for number, side in enumerate(sides):
            if step > 0 or number == 1:
                across(step, side).wait_send()
            for turn in range(2):
                sent(lambda: corner(step, side, turn), turn)
                sent(lambda: along_edge(step, turn, side), turn)
        for turn in range(2):
            sent(lambda: along_middle(step, turn), turn)

    for step in range(STEPS):
        final = step == STEPS - 1
        work = finish if final else collide_next
        if final:
            for earlier in range(step):
                all_sent(earlier)
            for side in range(2):
                kind_across(side).wait_send()
                for turn in range(2):
                    sent(lambda: kind_corner(side, turn), turn)
            for turn in range(2):
                sent(lambda: kind_along(turn), turn)

        def edge(number):
            side = sides[number]
            passed_edge_own(step, 1 - side)
            across(step, 1 - side).wait_recv()
            for turn in range(2):
                came(lambda: corner(step, 1 - side, turn), turn)
            passed_edge(step, 1 - side)
            x = last - last * side
            by_halves(lambda x, lanes: work(step, x, lanes), x, 1)
            if not final:
                stage_corners(step + 1, side)
                for turn in range(2):
                    go(lambda: corner(step + 1, side, turn), turn)
                stage_edge(step + 1, side)
                for turn in range(2):
                    go(lambda: along_edge(step + 1, turn, side), turn)
                across_go(step + 1, side)

        for turn in range(2):
            came(lambda: along_middle(step, turn), turn)
            came(lambda: along_edge(step, turn, sides[0]), turn)
        edge(0)
        for turn in range(2):
            came(lambda: along_edge(step, turn, sides[1]), turn)
        for x in range(1, last):
            passed_middle(step, x)
        by_halves(lambda x, lanes: work(step, x, lanes), 1, last - 1)
        if not final:
            for x in range(1, last):
                stage_rows(step + 1, x, range(9))
            for turn in range(2):
                go(lambda: along_middle(step + 1, turn), turn)
        edge(1)

    all_sent(STEPS - 1)


def local(populations, cell_kind, profile, vent_table, rates):
    _, _, depth, rows, cells = populations.shape
    half = cells // 2
    strip = 9 * depth
    f32, i32 = jnp.float32, jnp.int32
    anywhere = pl.BlockSpec(memory_space=pl.ANY)
    scalar = pl.BlockSpec(memory_space=pltpu.SMEM)
    return pl.pallas_call(
        kernel,
        out_shape=pltpu.VMEM(populations.shape, f32),
        in_specs=[anywhere, anywhere, anywhere, scalar, scalar],
        out_specs=pl.BlockSpec(memory_space=pltpu.VMEM),
        scratch_shapes=[
            pltpu.VMEM((27, depth, rows, cells), f32),
            pltpu.VMEM((STEPS, 27, depth, rows, cells), f32),
            pltpu.VMEM((27, depth, rows, cells), f32),
            pltpu.VMEM((27, depth, rows, cells), f32),
            pltpu.VMEM((3, depth, rows, cells), f32),
            pltpu.VMEM((54, rows, half), f32),
            pltpu.VMEM((depth, rows, cells), i32),
            pltpu.VMEM((depth, rows, cells), i32),
            pltpu.VMEM((2, rows, cells), i32),
            pltpu.VMEM((2, rows, cells), i32),
            pltpu.VMEM((4, depth + 2, rows, cells), f32),
            pltpu.VMEM((2, 4, rows, cells), f32),
            pltpu.VMEM((STEPS, 2, 9, rows, cells), f32),
            pltpu.VMEM((STEPS, 2, strip, 1, cells), f32),
            pltpu.VMEM((STEPS, 2, strip, 1, cells), f32),
            pltpu.VMEM((STEPS, 4, 3, 1, cells), f32),
            pltpu.VMEM((STEPS, 4, 3, 1, cells), f32),
            pltpu.VMEM((2, 2, rows, cells), i32),
            pltpu.VMEM((2, 2, rows, cells), i32),
            pltpu.VMEM((2, 2 * depth, 1, cells), i32),
            pltpu.VMEM((2, 2 * depth, 1, cells), i32),
            pltpu.VMEM((4, 2, 1, cells), i32),
            pltpu.VMEM((4, 2, 1, cells), i32),
            pltpu.SemaphoreType.DMA((depth + 2,)),
            pltpu.SemaphoreType.DMA((STEPS + 1, ROW)),
            pltpu.SemaphoreType.DMA((STEPS + 1, ROW)),
        ],
        compiler_params=pltpu.CompilerParams(collective_id=0, has_side_effects=True),
        name="lattice_steps",
    )(populations, cell_kind, profile, vent_table.T, rates)


def solution(mesh):
    return jax.shard_map(
        local,
        mesh=mesh,
        in_specs=(
            P("scen", "gx", None, None, None),
            P("gx", None, None, "scen"),
            P("gx", None, None, "scen"),
            P("scen", None),
            P(),
        ),
        out_specs=P("scen", "gx", None, None, None),
        check_vma=False,
    )
```

```python
import jax
import jax.numpy as jnp
from jax import lax
from jax.experimental import pallas as pl
from jax.experimental.pallas import tpu as pltpu
from jax.sharding import PartitionSpec as P

PY = 8
STEPS = 3
BIG = 1e30
MESH = pl.DeviceIdType.MESH

ACROSS, CORNER, ALONG, ROW = 0, 2, 6, 12


def direction(a, b, e):
    return 9 * (a + 1) + 3 * (b + 1) + (e + 1)


def digits(k):
    return (k // 9, k // 3 % 3, k % 3)


def forward(values):
    values = list(values)
    for stride in (1, 3, 9):
        for k in range(27):
            if k // stride % 3 == 0:
                low, mid, high = (values[k], values[k + stride], values[k + 2 * stride])
                both = low + high
                values[k] = both + 4.0 * mid
                values[k + stride] = high - low
                values[k + 2 * stride] = both
    return values


def backward(values):
    values = list(values)
    for stride in (9, 3, 1):
        for k in range(27):
            if k // stride % 3 == 0:
                zero, one, two = (values[k], values[k + stride], values[k + 2 * stride])
                values[k] = two - one
                values[k + stride] = zero - 0.5 * two
                values[k + 2 * stride] = two + one
    return values


def equilibrium_moments(density, velocity):
    share = [density]
    for _ in range(3):
        share.append(share[-1] * (1.0 / 3.0))
    triple = [3.0 * component * component for component in velocity]
    result = []
    for k in range(27):
        powers = digits(k)
        ones = [axis for axis in range(3) if powers[axis] == 1]
        twos = [axis for axis in range(3) if powers[axis] == 2]
        scale = share[len(twos)]
        if len(ones) == 0:
            shape = None
            for axis in twos:
                shape = 1.0 + triple[axis] if shape is None else shape + triple[axis]
            result.append(scale if shape is None else scale * shape)
        elif len(ones) == 3:
            result.append(None)
        else:
            shape = velocity[ones[0]]
            for axis in ones[1:]:
                shape = shape * velocity[axis]
            result.append(scale * shape)
    return result


def equilibrium(velocity):
    square = velocity[0] * velocity[0] + velocity[1] * velocity[1] + velocity[2] * velocity[2]
    base = 1.0 - 1.5 * square
    result = [None] * 27
    result[13] = base
    for k in range(13):
        projected = None
        for axis, digit in enumerate(digits(k)):
            if digit != 1:
                term = velocity[axis] if digit == 2 else -velocity[axis]
                projected = term if projected is None else projected + term
        even = base + 4.5 * projected * projected
        odd = 3.0 * projected
        result[k] = even + odd
        result[26 - k] = even - odd
    return result


def shifted(main, row, b, e, lane_count):
    if b != 0:
        count = main.shape[0]
        place = lax.broadcasted_iota(jnp.int32, main.shape, 0)
        moved = pltpu.roll(main, 1 if b == 1 else count - 1, 0)
        main = jnp.where(place == (0 if b == 1 else count - 1), row, moved)
    if e != 0:
        main = pltpu.roll(main, 1 if e == 1 else lane_count - 1, 1)
    return main


def kernel(
    populations, cell_kind, profile, vent_table, rates, out,
    start, collided, passed, walls, inlet, coef, kinds, profiles,
    rim_kinds, rim_profiles, fields, rim_fields,
    get_x, put_y, get_y, put_d, get_d,
    put_kx, get_kx, put_ky, get_ky, put_kd, get_kd,
    load_sem, send_sem, recv_sem,
):
    me = lax.axis_index("gx")
    count = lax.axis_size("gx")
    depth, rows, cells = collided.shape[2], collided.shape[3], collided.shape[4]
    last = depth - 1
    half = cells // 2
    row_place = lax.rem(me + PY // 2, PY)
    right_first = lax.rem((me + PY // 2) // PY, 2) == 1
    has_row = (row_place != PY - 1, row_place != 0)

    def device(side, turn):
        place = me + count
        if side is not None:
            place = place + (PY - 2 * PY * side)
        if turn is not None:
            place = place + (1 - 2 * turn)
        return lax.rem(place, count)

    barrier = pltpu.get_barrier_semaphore()
    for side in (None, 0, 1):
        for turn in (None, 0, 1):
            if side is not None or turn is not None:
                pl.semaphore_signal(
                    barrier, inc=1, device_id={"gx": device(side, turn)}, device_id_type=MESH
                )

    order = (0, last) + tuple(range(1, last))
    loads = {}
    for x in order:
        loads[x] = pltpu.make_async_copy(populations.at[:, 0, x], start.at[:, x], load_sem.at[x])
        loads[x].start()
    kind_load = pltpu.make_async_copy(cell_kind.at[0], kinds, load_sem.at[depth])
    profile_load = pltpu.make_async_copy(profile.at[0], profiles, load_sem.at[depth + 1])
    kind_load.start()
    profile_load.start()

    def remote(source, target_ref, slot, place, side, turn):
        return pltpu.make_async_remote_copy(
            src_ref=source,
            dst_ref=target_ref,
            send_sem=send_sem.at[slot, place],
            recv_sem=recv_sem.at[slot, place],
            device_id={"gx": device(side, turn)},
            device_id_type=MESH,
        )

    def across(step, side):
        source = collided.at[step, pl.ds(18 - 18 * side, 9), last - last * side]
        return remote(source, get_x.at[step, side], step, ACROSS + side, side, None)

    def across_go(step, side):
        for first in range(0, 9, 1):
            source = collided.at[step, pl.ds(18 - 18 * side + first, 1), last - last * side]
            target = get_x.at[step, side, pl.ds(first, 1)]
            remote(source, target, step, ACROSS + side, side, None).start()

    def corner(step, side, turn):
        place = 2 * side + turn
        return remote(
            put_d.at[step, place], get_d.at[step, place], step, CORNER + place, side, turn
        )

    def along(step, turn, first, size, place):
        part = pl.ds(first, size)
        return remote(
            put_y.at[step, turn, part], get_y.at[step, turn, part], step,
            ALONG + 3 * turn + place, None, turn,
        )

    def along_edge(step, turn, side):
        return along(step, turn, 9 * last - (9 * last - 3) * side, 6, 2 - 2 * side)

    def along_middle(step, turn):
        return along(step, turn, 9, 9 * (last - 1), 1)

    def kind_across(side):
        return remote(put_kx.at[side], get_kx.at[side], STEPS, ACROSS + side, side, None)

    def kind_corner(side, turn):
        place = 2 * side + turn
        return remote(
            put_kd.at[place], get_kd.at[place], STEPS, CORNER + place, side, turn
        )

    def kind_along(turn):
        return remote(put_ky.at[turn], get_ky.at[turn], STEPS, ALONG + turn, None, turn)

    def go(copy, turn):
        @pl.when(has_row[turn])
        def _():
            copy().start()

    def sent(copy, turn):
        @pl.when(has_row[turn])
        def _():
            copy().wait_send()

    def came(copy, turn):
        @pl.when(has_row[1 - turn])
        def _():
            copy().wait_recv()

    for k in range(27):
        scale = 1.0
        for digit in digits(k):
            scale = scale * (0.25 if digit == 0 else 0.5)
        rate = rates[k]
        coef[2 * k] = jnp.full((rows, half), scale * (1.0 - rate), jnp.float32)
        coef[2 * k + 1] = jnp.full((rows, half), scale * rate, jnp.float32)

    def relaxed(moments, target):
        result = []
        for k in range(27):
            value = coef[2 * k] * moments[k]
            if target[k] is not None:
                value = value + coef[2 * k + 1] * target[k]
            result.append(value)
        return backward(result)

    def collide_first(x, lanes):
        moments = forward([start[k, x, :, lanes] for k in range(27)])
        density = moments[0]
        velocity = [moments[k] / density for k in (9, 3, 1)]
        result = relaxed(moments, equilibrium_moments(density, velocity))
        for k in range(27):
            collided[0, k, x, :, lanes] = result[k]

    def cell_state(step, x, lanes):
        values = [
            collided[step, k, x, :, lanes] if k == 13 else passed[k, x, :, lanes]
            for k in range(27)
        ]
        moments = forward(values)
        velocity = [moments[k] / moments[0] for k in (9, 3, 1)]
        return (values, moments, velocity, kinds[x, :, lanes])

    def collide_next(step, x, lanes):
        values, moments, velocity, kind = cell_state(step, x, lanes)
        fluid = kind == 0
        moving = fluid | (kind == 4)
        velocity = [
            jnp.where(moving, velocity[axis], inlet[axis, x, :, lanes]) for axis in range(3)
        ]
        density = jnp.where(fluid, moments[0], 216.0)
        target = equilibrium_moments(density, velocity)
        moments = [
            jnp.where(fluid, moments[k], 0.0 if target[k] is None else target[k])
            for k in range(27)
        ]
        result = relaxed(moments, target)
        for k in range(27):
            collided[step + 1, k, x, :, lanes] = result[k]

    def finish(step, x, lanes):
        values, moments, velocity, kind = cell_state(step, x, lanes)
        fluid = kind == 0
        velocity = [
            jnp.where(kind == 4, velocity[axis], inlet[axis, x, :, lanes]) for axis in range(3)
        ]
        forced = equilibrium(velocity)
        for k in range(27):
            out[k, 0, x, :, lanes] = jnp.where(fluid, values[k], forced[k])

    def by_halves(work, first, planes):
        def body(index, carry):
            plane = first + index // 2
            lanes = pl.ds(pl.multiple_of(index % 2 * half, half), half)
            work(plane, lanes)
            return carry

        lax.fori_loop(0, 2 * planes, body, 0)

    def stage_corners(step, side):
        x = last - last * side
        for turn in range(2):
            y = rows - 1 if turn == 0 else 0
            for e in range(3):
                k = 18 - 18 * side + (6 - 6 * turn) + e
                put_d[step, 2 * side + turn, e] = collided[step, k, x, pl.ds(y, 1), :]

    def stage_rows(step, x, pairs):
        for turn in range(2):
            y = rows - 1 if turn == 0 else 0
            for pair in pairs:
                k = 9 * (pair // 3) + (6 - 6 * turn) + pair % 3
                put_y[step, turn, 9 * x + pair] = collided[step, k, x, pl.ds(y, 1), :]

    def stage_edge(step, side):
        x = last - last * side
        for turn in range(2):
            y = rows - 1 if turn == 0 else 0
            for pair in range(6):
                k = 9 * (pair // 3) + 9 * side + (6 - 6 * turn) + pair % 3
                row = 9 * last - (9 * last - 3) * side + pair
                put_y[step, turn, row] = collided[step, k, x, pl.ds(y, 1), :]

    def passed_on(step, k, x, opposite, main, row, b, e):
        source = shifted(main, row, b, e, cells)
        wall = walls[k, x]
        passed[k, x] = jnp.where(wall > 0.5 * BIG, source, collided[step, opposite, x] + wall)

    def passed_middle(step, x):
        for k in range(27):
            if k == 13:
                continue
            a, b, e = (digit - 1 for digit in digits(k))
            row = None
            if b != 0:
                row = get_y[step, (1 - b) // 2, 9 * (x - a) + 3 * (a + 1) + (e + 1)]
            passed_on(step, k, x, 26 - k, collided[step, k, x - a], row, b, e)

    def passed_edge_own(step, side):
        x = last * side
        into, back = (18 - 18 * side, 18 * side)
        inner = x + 1 - 2 * side
        for b in (-1, 0, 1):
            turn = (1 - b) // 2
            for e in (-1, 0, 1):
                place = 3 * (b + 1) + (e + 1)
                row = None
                if b != 0 or e != 0:
                    if b != 0:
                        row = get_y[step, turn, 9 * x + 3 + (e + 1)]
                    passed_on(
                        step, 9 + place, x, 17 - place, collided[step, 9 + place, x], row, b, e
                    )
                if b != 0:
                    row = get_y[step, turn, 9 * inner + 6 * side + (e + 1)]
                passed_on(
                    step, back + place, x, into + (8 - place),
                    collided[step, back + place, inner], row, b, e,
                )

    def passed_edge(step, side):
        x = last * side
        into, back = (18 - 18 * side, 18 * side)
        for b in (-1, 0, 1):
            turn = (1 - b) // 2
            for e in (-1, 0, 1):
                place = 3 * (b + 1) + (e + 1)
                row = None
                if b != 0:
                    row = get_d[step, 2 * side + turn, e + 1]
                passed_on(
                    step, into + place, x, back + (8 - place), get_x[step, side, place], row, b, e
                )

    def field_values(kind, index):
        velocity = [jnp.zeros(kind.shape, jnp.float32) for _ in range(3)]
        for entry in range(vent_table.shape[1]):
            chosen = index == entry
            for axis in range(3):
                velocity[axis] = jnp.where(chosen, vent_table[axis, entry], velocity[axis])
        is_open = (kind == 0) | (kind >= 3)
        vent = kind == 2
        result = [jnp.where(is_open, BIG, 0.0)]
        for axis in range(3):
            result.append(jnp.where(vent, velocity[axis], 0.0))
        return result, velocity

    def wall_part(plane, b):
        lane = lax.broadcasted_iota(jnp.int32, (rows, cells), 1)
        for e in (-1, 0, 1):
            moved = []
            for field in range(4):
                row = None
                if b != 0:
                    row = rim_fields[0 if b == 1 else 1, field, pl.ds(plane, 1), :]
                value = shifted(fields[field, plane], row, b, e, cells)
                if e != 0:
                    value = jnp.where(lane == (0 if e == 1 else cells - 1), 0.0, value)
                moved.append(value)
            cross = moved[0]
            if b != 0:
                cross = cross + (6.0 * b) * moved[2]
            if e != 0:
                cross = cross + (6.0 * e) * moved[3]
            for a in (-1, 0, 1):
                x = plane - 1 + a
                k = direction(a, b, e)
                if 0 <= x <= last and k != 13:
                    walls[k, x] = cross if a == 0 else cross + (6.0 * a) * moved[1]

    def prepare_fields():
        for x in range(depth):
            values, velocity = field_values(kinds[x], profiles[x])
            for field in range(4):
                fields[field, x + 1] = values[field]
            for axis in range(3):
                inlet[axis, x] = jnp.where(kinds[x] == 3, velocity[axis], 0.0)

    def prepare_walls():
        for plane, side in ((0, 0), (depth + 1, 1)):
            values, _ = field_values(get_kx[side, 0], get_kx[side, 1])
            for field in range(4):
                fields[field, plane] = values[field]
        for side in range(2):
            for target, shift in ((rim_kinds, 0), (rim_profiles, 1)):
                target[side] = jnp.zeros((rows, cells), jnp.int32)
                for x in range(depth):
                    target[side, pl.ds(x + 1, 1), :] = get_ky[side, shift * depth + x]
                for row, place in ((0, side), (depth + 1, 2 + side)):
                    target[side, pl.ds(row, 1), :] = get_kd[place, shift]
            outside = row_place == (0 if side == 0 else PY - 1)
            kind = jnp.where(outside, 1, rim_kinds[side])
            values, _ = field_values(kind, rim_profiles[side])
            for field in range(4):
                rim_fields[side, field] = values[field]
        for plane in range(depth + 2):
            for b in (-1, 0, 1):
                if b != 0 or plane in (0, depth + 1):
                    wall_part(plane, b)

    for x in order:
        loads[x].wait()
        by_halves(collide_first, x, 1)
    for side in range(2):
        stage_corners(0, side)
        stage_edge(0, side)
    for x in range(1, last):
        stage_rows(0, x, range(9))
    kind_load.wait()
    profile_load.wait()
    for side, x in ((0, last), (1, 0)):
        put_kx[side, 0] = kinds[x]
        put_kx[side, 1] = profiles[x]
        for turn in range(2):
            y = rows - 1 if turn == 0 else 0
            put_kd[2 * side + turn, 0] = kinds[x, pl.ds(y, 1), :]
            put_kd[2 * side + turn, 1] = profiles[x, pl.ds(y, 1), :]
    for turn in range(2):
        y = rows - 1 if turn == 0 else 0
        for x in range(depth):
            put_ky[turn, x] = kinds[x, pl.ds(y, 1), :]
            put_ky[turn, depth + x] = profiles[x, pl.ds(y, 1), :]

    early = jnp.where(right_first, 0, 1)
    sides = (early, 1 - early)
    pl.semaphore_wait(barrier, 8)
    for side in sides:
        kind_across(side).start()
        for turn in range(2):
            go(lambda: kind_corner(side, turn), turn)
    for turn in range(2):
        go(lambda: kind_along(turn), turn)
    for number, side in enumerate(sides):
        if number == 1:
            across(0, sides[0]).wait_send()
        for turn in range(2):
            go(lambda: corner(0, side, turn), turn)
        across_go(0, side)
        if number == 0:
            for turn in range(2):
                go(lambda: along_middle(0, turn), turn)
                go(lambda: along_edge(0, turn, sides[0]), turn)
                go(lambda: along_edge(0, turn, sides[1]), turn)

    prepare_fields()
    for plane in range(1, depth + 1):
        wall_part(plane, 0)
    for side in sides:
        kind_across(side).wait_recv()
        for turn in range(2):
            came(lambda: kind_corner(side, turn), turn)
    for turn in range(2):
        came(lambda: kind_along(turn), turn)
    prepare_walls()

    def all_sent(step):
        for number, side in enumerate(sides):
            if step > 0 or number == 1:
                across(step, side).wait_send()
            for turn in range(2):
                sent(lambda: corner(step, side, turn), turn)
                sent(lambda: along_edge(step, turn, side), turn)
        for turn in range(2):
            sent(lambda: along_middle(step, turn), turn)

    for step in range(STEPS):
        final = step == STEPS - 1
        work = finish if final else collide_next
        if final:
            for earlier in range(step):
                all_sent(earlier)
            for side in range(2):
                kind_across(side).wait_send()
                for turn in range(2):
                    sent(lambda: kind_corner(side, turn), turn)
            for turn in range(2):
                sent(lambda: kind_along(turn), turn)

        def edge(number):
            side = sides[number]
            passed_edge_own(step, 1 - side)
            across(step, 1 - side).wait_recv()
            for turn in range(2):
                came(lambda: corner(step, 1 - side, turn), turn)
            passed_edge(step, 1 - side)
            x = last - last * side
            by_halves(lambda x, lanes: work(step, x, lanes), x, 1)
            if not final:
                stage_corners(step + 1, side)
                for turn in range(2):
                    go(lambda: corner(step + 1, side, turn), turn)
                stage_edge(step + 1, side)
                for turn in range(2):
                    go(lambda: along_edge(step + 1, turn, side), turn)
                across_go(step + 1, side)

        for turn in range(2):
            came(lambda: along_middle(step, turn), turn)
            came(lambda: along_edge(step, turn, sides[0]), turn)
        edge(0)
        for turn in range(2):
            came(lambda: along_edge(step, turn, sides[1]), turn)
        for x in range(1, last):
            passed_middle(step, x)
        by_halves(lambda x, lanes: work(step, x, lanes), 1, last - 1)
        if not final:
            for x in range(1, last):
                stage_rows(step + 1, x, range(9))
            for turn in range(2):
                go(lambda: along_middle(step + 1, turn), turn)
        edge(1)

    all_sent(STEPS - 1)


def local(populations, cell_kind, profile, vent_table, rates):
    _, _, depth, rows, cells = populations.shape
    half = cells // 2
    strip = 9 * depth
    f32, i32 = jnp.float32, jnp.int32
    anywhere = pl.BlockSpec(memory_space=pl.ANY)
    scalar = pl.BlockSpec(memory_space=pltpu.SMEM)
    return pl.pallas_call(
        kernel,
        out_shape=pltpu.VMEM(populations.shape, f32),
        in_specs=[anywhere, anywhere, anywhere, scalar, scalar],
        out_specs=pl.BlockSpec(memory_space=pltpu.VMEM),
        scratch_shapes=[
            pltpu.VMEM((27, depth, rows, cells), f32),
            pltpu.VMEM((STEPS, 27, depth, rows, cells), f32),
            pltpu.VMEM((27, depth, rows, cells), f32),
            pltpu.VMEM((27, depth, rows, cells), f32),
            pltpu.VMEM((3, depth, rows, cells), f32),
            pltpu.VMEM((54, rows, half), f32),
            pltpu.VMEM((depth, rows, cells), i32),
            pltpu.VMEM((depth, rows, cells), i32),
            pltpu.VMEM((2, rows, cells), i32),
            pltpu.VMEM((2, rows, cells), i32),
            pltpu.VMEM((4, depth + 2, rows, cells), f32),
            pltpu.VMEM((2, 4, rows, cells), f32),
            pltpu.VMEM((STEPS, 2, 9, rows, cells), f32),
            pltpu.VMEM((STEPS, 2, strip, 1, cells), f32),
            pltpu.VMEM((STEPS, 2, strip, 1, cells), f32),
            pltpu.VMEM((STEPS, 4, 3, 1, cells), f32),
            pltpu.VMEM((STEPS, 4, 3, 1, cells), f32),
            pltpu.VMEM((2, 2, rows, cells), i32),
            pltpu.VMEM((2, 2, rows, cells), i32),
            pltpu.VMEM((2, 2 * depth, 1, cells), i32),
            pltpu.VMEM((2, 2 * depth, 1, cells), i32),
            pltpu.VMEM((4, 2, 1, cells), i32),
            pltpu.VMEM((4, 2, 1, cells), i32),
            pltpu.SemaphoreType.DMA((depth + 2,)),
            pltpu.SemaphoreType.DMA((STEPS + 1, ROW)),
            pltpu.SemaphoreType.DMA((STEPS + 1, ROW)),
        ],
        compiler_params=pltpu.CompilerParams(collective_id=0, has_side_effects=True),
        name="lattice_steps",
    )(populations, cell_kind, profile, vent_table.T, rates)


def solution(mesh):
    return jax.shard_map(
        local,
        mesh=mesh,
        in_specs=(
            P("scen", "gx", None, None, None),
            P("gx", None, None, "scen"),
            P("gx", None, None, "scen"),
            P("scen", None),
            P(),
        ),
        out_specs=P("scen", "gx", None, None, None),
        check_vma=False,
    )
```
